256 devices in a mesh: gx: 8 (over z), gy: 8 (over y, core), gz: 4 (over x).
Axes of the slice: x: 4, y: 4, z: 8, core: 2. Of those that a mesh axis runs over, the one named last changes fastest.
Arguments:
- density: float32 [64, 64, 512], P('gx', 'gy', 'gz'), may hold values from 0.5 to 2
- base_velocity: float32 [3, 64, 64, 512], P(None, 'gx', 'gy', 'gz'), may hold values from -0.4 to 0.4
- cells: int32 [3, 65536], P(None, ('gx', 'gy', 'gz')), may hold values from 0 to 511, as said below
- offsets: float32 [3, 65536], P(None, ('gx', 'gy', 'gz')), may hold values from 0 to 1
- target: float32 [3, 65536], P(None, ('gx', 'gy', 'gz')), may hold values from -0.4 to 0.4
- stiffness: float32 [65536], P(('gx', 'gy', 'gz')), may hold values from 0.01 to 0.1
- counts: int32 [256], P(('gx', 'gy', 'gz')), may hold values from 1 to 256, as said below
Outputs:
- forces: float32 [3, 65536], P(None, ('gx', 'gy', 'gz'))
The draws below stay inside these ranges and needn't reach their ends.
Inputs may be any that keep to these rules, and one draw needn't show every extreme that they name: `cells`: each marker's cell lies inside the lattice block of the device that holds its slot. `counts`: some device holds exactly 256 live markers in every draw.
All inputs are finite; a program needn't handle non-finite values.
Results may differ from the reference program's by a relative error of at most 0.0001.
Values sent between devices are 32-bit elements; how exact they have to be, the bound alone decides.
A program may use at most 64 MiB of HBM per device.

```python
import math
import jax
import jax.numpy as jnp
from jax import lax

CX = 8
CY = 8
CZ = 128
CAP = 256
ITERS = 3
NX = 64
NY = 64
NZ = 512
SLOTS = 65536
DEVICES = 256


def draw_cells(key, part):
    blocks_y = NY // CY
    blocks_z = NZ // CZ
    device = jnp.arange(SLOTS, dtype=jnp.int32) // CAP
    block_x = device // (blocks_y * blocks_z)
    block_y = device // blocks_z % blocks_y
    block_z = device % blocks_z
    keys = jax.random.split(key, 3)
    inside_x = jax.random.randint(keys[0], (SLOTS,), 0, CX, dtype=jnp.int32)
    inside_y = jax.random.randint(keys[1], (SLOTS,), 0, CY, dtype=jnp.int32)
    inside_z = jax.random.randint(keys[2], (SLOTS,), 0, CZ, dtype=jnp.int32)
    return jnp.stack([block_x * CX + inside_x, block_y * CY + inside_y, block_z * CZ + inside_z]).astype(jnp.int32)


def draw_counts(key, part):
    keys = jax.random.split(key, 3)
    divisor = 1 + jax.random.randint(keys[0], (DEVICES,), 0, 6, dtype=jnp.int32)
    jitter = jax.random.randint(keys[1], (DEVICES,), 0, CAP // 8 + 1, dtype=jnp.int32)
    loads = jnp.maximum(CAP // divisor - jitter, 1)
    fullest = jax.random.randint(keys[2], (), 0, DEVICES, dtype=jnp.int32)
    loads = jnp.where(jnp.arange(DEVICES, dtype=jnp.int32) == fullest, CAP, loads)
    return loads.astype(jnp.int32)


def levels(stream_key, extent, shards, low, largest):
    level, own = 1.0, jax.random.fold_in(stream_key, 6)
    for axis_at, blocks in shards:
        steps = jnp.exp(jax.random.uniform(jax.random.fold_in(own, axis_at), (blocks,), jnp.float32, low / len(shards), largest / len(shards)))
        level = level * jnp.repeat(steps, extent[axis_at] // blocks).reshape([-1 if axis == axis_at else 1 for axis in range(len(extent))])
    return level


def normal_values(stream_key, dims, scale, limit, shards=(), kind=jnp.bfloat16):
    values = scale * jax.random.normal(stream_key, dims, jnp.float32)
    if shards:
        values = values * levels(stream_key, dims, shards, -0.22, 0.18)
    return jnp.clip(values, -limit, limit).astype(kind)


def setup_inputs(seed: int = 0) -> dict:
    seeds = jax.random.split(jax.random.key(seed), 8)
    return {
        "density": jnp.clip(jnp.exp(math.log(2.0) - 1.3862944 * jax.random.uniform(seeds[0], (NX, NY, NZ), jnp.float32) ** levels(seeds[0], (NX, NY, NZ), ((0, 8), (1, 8), (2, 4)), -0.2, 0.2)), 0.5, 2.0),
        "base_velocity": normal_values(seeds[1], (3, NX, NY, NZ), 0.05, 0.4, ((1, 8), (2, 8), (3, 4)), jnp.float32),
        "cells": draw_cells(jax.random.fold_in(seeds[7], 71), 0),
        "offsets": jnp.clip(1.0 * jax.random.uniform(seeds[3], (3, SLOTS), jnp.float32) ** levels(seeds[3], (3, SLOTS), ((1, 256),), -0.2, 0.2), 0.0, 1.0),
        "target": normal_values(seeds[4], (3, SLOTS), 0.05, 0.4, ((1, 256),), jnp.float32),
        "stiffness": jnp.clip(jnp.exp(math.log(0.1) - 2.3025851 * jax.random.uniform(seeds[5], (SLOTS,), jnp.float32) ** levels(seeds[5], (SLOTS,), ((0, 256),), -0.2, 0.2)), 0.01, 0.1),
        "counts": draw_counts(jax.random.fold_in(seeds[7], 71), 0),
    }


def moving_directions():
    listing = []
    for along_x in (-1, 0, 1):
        for along_y in (-1, 0, 1):
            for along_z in (-1, 0, 1):
                order = abs(along_x) + abs(along_y) + abs(along_z)
                if order == 1:
                    listing.append((along_x, along_y, along_z, 1.0 / 18.0))
                elif order == 2:
                    listing.append((along_x, along_y, along_z, 1.0 / 36.0))
    return listing

def delta_weights(fraction):

    def inner(radius):
        return (3.0 - 2.0 * radius + jnp.sqrt(1.0 + 4.0 * radius - 4.0 * radius * radius)) / 8.0

    def outer(radius):
        return (5.0 - 2.0 * radius - jnp.sqrt(-7.0 + 12.0 * radius - 4.0 * radius * radius)) / 8.0
    return jnp.stack([outer(1.0 + fraction), inner(fraction), inner(1.0 - fraction), outer(2.0 - fraction)])

def reference(density, base_velocity, cells, offsets, target, stiffness, counts):
    live = (jnp.arange(CAP, dtype=jnp.int32)[None, :] < counts[:, None]).reshape(-1).astype(jnp.float32)
    scale = lax.rsqrt(density)
    weight_x = delta_weights(offsets[0])
    weight_y = delta_weights(offsets[1])
    weight_z = delta_weights(offsets[2])
    index_x = [((cells[0] + shift - 1) % NX).astype(jnp.int32) for shift in range(4)]
    index_y = [((cells[1] + shift - 1) % NY).astype(jnp.int32) for shift in range(4)]
    index_z = [((cells[2] + shift - 1) % NZ).astype(jnp.int32) for shift in range(4)]
    directions = moving_directions()

    def interpolate(field):
        total = jnp.zeros((3, SLOTS), jnp.float32)
        for first in range(4):
            for second in range(4):
                for third in range(4):
                    weight = weight_x[first] * weight_y[second] * weight_z[third]
                    total = total + field[:, index_x[first], index_y[second], index_z[third]] * weight
        return total

    def spread(vector):
        grid = jnp.zeros((3, NX, NY, NZ), jnp.float32)
        for first in range(4):
            for second in range(4):
                for third in range(4):
                    weight = weight_x[first] * weight_y[second] * weight_z[third]
                    grid = grid.at[:, index_x[first], index_y[second], index_z[third]].add(vector * weight)
        return grid

    def apply(vector):
        moved = scale * spread(vector)
        post = [jnp.zeros((NX, NY, NZ), jnp.float32) for component in range(3)]
        for along_x, along_y, along_z, share in directions:
            population = 3.0 * share * (along_x * moved[0] + along_y * moved[1] + along_z * moved[2])
            shifted = jnp.roll(population, (along_x, along_y, along_z), axis=(0, 1, 2))
            for component, along in enumerate((along_x, along_y, along_z)):
                if along != 0:
                    post[component] = post[component] + along * shifted
        velocity = scale * (moved + jnp.stack(post)) * 0.5
        return live * (interpolate(velocity) + stiffness * vector)
    right = live * (target - interpolate(base_velocity))
    solution = jnp.zeros_like(right)
    residual = right
    direction = right
    norm_now = jnp.sum(residual * residual)
    for step in range(ITERS):
        image = apply(direction)
        alpha = norm_now / jnp.sum(direction * image)
        solution = solution + alpha * direction
        residual = residual - alpha * image
        norm_next = jnp.sum(residual * residual)
        direction = residual + norm_next / norm_now * direction
        norm_now = norm_next
    return solution
```

```python
import functools

import jax
import jax.numpy as jnp
from jax import lax
from jax.experimental import pallas as pl
from jax.experimental.pallas import tpu as pltpu
from jax.sharding import PartitionSpec as P

ITERS = 3
CX, CY, CZ = 8, 8, 128
CAP = 256
WX, WY, WZ = 13, 16, 256
TZ = 144
AXES = ("gx", "gy", "gz")
ALL = ("gx", "gy", "gz")
MESH = pl.DeviceIdType.MESH
SHIFT = 0.1
F32, BF16 = jnp.float32, jnp.bfloat16

GROUPS = [(dx, dy) for dx in (-1, 0, 1) for dy in (-1, 0, 1)]
DZS = (-1, 1, 0)
ORDER = sorted(range(9), key=lambda g: abs(GROUPS[g][0]) + abs(GROUPS[g][1]))
PLANES = {-1: (0, 4), 0: (1, 12), 1: (9, 4)}
ROWS = {-1: (0, 8), 0: (0, 16), 1: (8, 8)}
TAKE = {-1: (6, 8), 0: (0, 8), 1: (0, 3)}


def group_of(dx, dy):
    return (dx + 1) * 3 + dy + 1


def slot_of(dx, dy, dz):
    return group_of(dx, dy) * 3 + DZS.index(dz)


NEIGHBOURS = [
    (GROUPS[g][0], GROUPS[g][1], dz)
    for g in ORDER
    for dz in DZS
    if (GROUPS[g][0], GROUPS[g][1], dz) != (0, 0, 0)
]
CENTRE = group_of(0, 0)
SPANS = [PLANES[dx][1] * ROWS[dy][1] for dx, dy in GROUPS]
STARTS = [sum(SPANS[:g]) for g in range(9)]


def split(value):
    high = value.astype(BF16)
    return high, (value - high.astype(F32)).astype(BF16)


def dot3(lh, ll, rh, rl, dims):
    dot = functools.partial(
        lax.dot_general, dimension_numbers=(dims, ((), ())), preferred_element_type=F32
    )
    return dot(lh, rh) + (dot(ll, rh) + dot(lh, rl))


def kernel(
    sizes,
    density_ref, base_ref, cells_ref, offsets_ref, target_ref, stiff_ref, counts_ref,
    out_ref,
    field, ftrans, pack_z, mark_own, recv_f, recv_z, marks, main, halo, ztile, wide,
    table_h, table_l, own_h, own_l, wxy, left_h, left_l, grid, moved, plane_a, plane_b, plane_c,
    vel_h, vel_l, vecs, images, recv_v, part, recv_a, part_b, recv_b,
    send_f, got_f, send_z, got_z, send_m, got_m, send_v, got_v, send_r, got_r,
):
    size_x, size_y, size_z = sizes
    ix, iy, iz = (lax.axis_index(a) for a in AXES)

    def at(dx, dy, dz):
        return (
            lax.rem(ix + dx + size_x, size_x),
            lax.rem(iy + dy + size_y, size_y),
            lax.rem(iz + dz + size_z, size_z),
        )

    def mate(k):
        rest = lax.rem(iy * size_z + iz + k, size_y * size_z)
        return (ix, rest // size_z, lax.rem(rest, size_z))

    def along(k):
        return (lax.rem(ix + k, size_x), iy, iz)

    barrier = pltpu.get_barrier_semaphore()
    for offset in NEIGHBOURS:
        pl.semaphore_signal(barrier, inc=1, device_id=at(*offset), device_id_type=MESH)

    def greet_mate(k, carry):
        pl.semaphore_signal(barrier, inc=1, device_id=mate(k), device_id_type=MESH)
        return carry

    lax.fori_loop(1, size_y * size_z, greet_mate, 0)
    for k in range(1, size_x):
        pl.semaphore_signal(barrier, inc=1, device_id=along(k), device_id_type=MESH)

    field[0:3] = base_ref[...]
    field[3] = lax.rsqrt(density_ref[...])
    ftrans[...] = field[...].reshape(4 * CX * CY, CZ).T
    pack_z[0:2] = ftrans[CZ - 2 : CZ]
    pack_z[2:8] = ftrans[0:6]
    anchors = (ix * CX, iy * CY, iz * CZ)
    for k in range(3):
        mark_own[k : k + 1] = (cells_ref[k : k + 1] - anchors[k]).astype(F32)
    mark_own[3:6] = offsets_ref[...]
    mark_own[6:8] = jnp.zeros((2, CAP), F32)
    marks[slot_of(0, 0, 0)] = mark_own[...]

    pl.semaphore_wait(barrier, len(NEIGHBOURS) + size_y * size_z - 1 + size_x - 1)

    def remote(src, dst, send, recv, device):
        return pltpu.make_async_remote_copy(
            src_ref=src, dst_ref=dst, send_sem=send, recv_sem=recv, device_id=device,
            device_id_type=MESH,
        )

    def drain(ref, sem):
        pltpu.make_async_copy(ref, ref, sem).wait()

    def halo_copy(dx, dy):
        a, b = TAKE[-dx]
        g = group_of(-dx, -dy)
        return remote(
            field.at[:, a:b], recv_f.at[g, :, a:b], send_f.at[g], got_f.at[g], at(dx, dy, 0)
        )

    for dx, dy in GROUPS:
        if (dx, dy) != (0, 0):
            halo_copy(dx, dy).start()
    for dx, dy, dz in NEIGHBOURS:
        back = slot_of(-dx, -dy, -dz)
        if dz:
            remote(
                pack_z, recv_z.at[group_of(-dx, -dy) * 2 + DZS.index(-dz)], send_z, got_z, at(dx, dy, dz)
            ).start()
        remote(mark_own, marks.at[back], send_m, got_m, at(dx, dy, dz)).start()

    table_h[...] = jnp.zeros(table_h.shape, BF16)
    table_l[...] = jnp.zeros(table_l.shape, BF16)
    own_h[...] = jnp.zeros(own_h.shape, BF16)
    own_l[...] = jnp.zeros(own_l.shape, BF16)
    ztile[...] = jnp.zeros(ztile.shape, F32)
    main[:, :, 8:16] = jnp.zeros((4, WX, 8, CZ), F32)
    halo[:, :, 8:16] = jnp.zeros((4, WX, 8, CZ), F32)
    grid[...] = jnp.zeros(grid.shape, F32)
    vecs[...] = jnp.zeros(vecs.shape, F32)

    live = (lax.broadcasted_iota(jnp.int32, (1, CAP), 1) < counts_ref[0]).astype(F32)
    stiff = stiff_ref[...]

    def axis_table(first, rows, start, weights):
        away = (
            lax.broadcasted_iota(jnp.int32, (rows, CAP), 0).astype(F32) + float(first) - start
        )
        value = jnp.zeros((rows, CAP), F32)
        for step in range(4):
            value = jnp.where(away == float(step), weights[step], value)
        return value

    def build(g, j):
        (dx, dy), dz = GROUPS[g], DZS[j]
        mark = marks[g * 3 + j]
        fraction = mark[3:6]
        root = jnp.sqrt(1.0 + 4.0 * fraction - 4.0 * fraction * fraction)
        weights = [
            (3.0 - 2.0 * fraction - root) * 0.125,
            (3.0 - 2.0 * fraction + root) * 0.125,
            (1.0 + 2.0 * fraction + root) * 0.125,
            (1.0 + 2.0 * fraction - root) * 0.125,
        ]
        of = lambda k: [w[k : k + 1] for w in weights]
        x0, nx = PLANES[dx]
        y0, ny = ROWS[dy]
        table_x = axis_table(x0, 16, mark[0:1] + float(1 + CX * dx), of(0))
        table_y = axis_table(y0, ny, mark[1:2] + float(1 + CY * dy), of(1))
        lanes = slice(j * CAP, (j + 1) * CAP)
        for x in range(nx):
            at_row = STARTS[g] + x * ny
            wxy[at_row : at_row + ny, lanes] = table_x[x : x + 1] * table_y
        z0, nz = {-1: (0, 16), 0: (0, TZ), 1: (CZ, 16)}[dz]
        high, low = split(axis_table(z0, nz, mark[2:3] + float(1 + CZ * dz), of(2)))
        table_h[g, z0 : z0 + nz, lanes] = high
        table_l[g, z0 : z0 + nz, lanes] = low
        if g == CENTRE and dz == 0:
            own_h[0:TZ] = high
            own_l[0:TZ] = low

    build(CENTRE, 2)

    for g, (dx, dy) in enumerate(GROUPS):
        if g != CENTRE:
            halo_copy(-dx, -dy).wait_recv()
    drain(recv_z, got_z)
    low_rows = lax.broadcasted_iota(jnp.int32, (8, 4 * CX * CY), 0) < 2
    for g, (dx, dy) in enumerate(GROUPS):
        (xa, xb), (ya, yb) = TAKE[dx], TAKE[dy]
        x0, y0 = xa + CX * dx + 2, ya + CY * dy + 2
        source = field if g == CENTRE else recv_f.at[g]
        main[:, x0 : x0 + xb - xa, y0 : y0 + yb - ya] = source[:, xa:xb, ya:yb]
        columns = jnp.where(low_rows, recv_z[2 * g], recv_z[2 * g + 1])
        ztile[:, :, :, 0:8] = columns.T.reshape(4, CX, CY, 8)
        halo[:, x0 : x0 + xb - xa, y0 : y0 + yb - ya] = ztile[:, xa:xb, ya:yb]
    lane = lax.broadcasted_iota(jnp.int32, (WY, CZ), 1)

    def widen(x, carry):
        for c in range(4):
            turned = pltpu.roll(main[c, x], 2, 1)
            edge = halo[c, x]
            wide[c, x, :, 0:CZ] = jnp.where(lane < 2, edge, turned)
            wide[c, x, :, CZ:] = jnp.where(lane < 2, turned, jnp.where(lane < 5, edge, 0.0))
        return carry

    lax.fori_loop(0, WX, widen, 0)

    def interpolate():
        high = vel_h[...].reshape(3 * 11 * WY, WZ)
        low = vel_l[...].reshape(3 * 11 * WY, WZ)
        rows = dot3(high, low, own_h[...], own_l[...], ((1,), (0,)))
        weight = wxy[STARTS[CENTRE] : STARTS[CENTRE] + 11 * WY, 2 * CAP : 3 * CAP]
        return [
            jnp.sum(rows[c * 11 * WY : (c + 1) * 11 * WY] * weight, axis=0, keepdims=True)
            for c in range(3)
        ]

    for c in range(3):
        high, low = split(wide[c, 1:12])
        vel_h[c] = high
        vel_l[c] = low
    for c, value in enumerate(interpolate()):
        vecs[0, c : c + 1] = live * (target_ref[c : c + 1] - value)

    drain(marks.at[0:26], got_m)

    def send_vector(a):
        for dx, dy, dz in NEIGHBOURS:
            back = slot_of(-dx, -dy, -dz)
            remote(
                vecs.at[a], recv_v.at[a, back], send_v.at[a], got_v.at[a, back // 3], at(dx, dy, dz)
            ).start()
        recv_v[a, slot_of(0, 0, 0)] = vecs[a]

    def spread(a):
        grid[:, :, :, 0:TZ] = jnp.zeros((3, WX, WY, TZ), F32)
        for g in ORDER:
            (dx, dy) = GROUPS[g]
            if g == CENTRE:
                drain(recv_v.at[a, 3 * g : 3 * g + 2], got_v.at[a, g])
            else:
                drain(recv_v.at[a, 3 * g : 3 * g + 3], got_v.at[a, g])
            span = SPANS[g]
            for j in range(3):
                lanes = slice(j * CAP, (j + 1) * CAP)
                vector = recv_v[a, 3 * g + j]
                weight = wxy[STARTS[g] : STARTS[g] + span, lanes]
                for c in range(3):
                    high, low = split(weight * vector[c : c + 1])
                    left_h[c * span : (c + 1) * span, lanes] = high
                    left_l[c * span : (c + 1) * span, lanes] = low
            total = dot3(
                left_h[0 : 3 * span], left_l[0 : 3 * span], table_h[g], table_l[g], ((1,), (1,))
            )
            x0, nx = PLANES[dx]
            y0, ny = ROWS[dy]
            for c in range(3):
                at_place = (c, slice(x0, x0 + nx), slice(y0, y0 + ny), slice(0, TZ))
                grid[at_place] += total[c * span : (c + 1) * span].reshape(nx, ny, TZ)

    def shifts(value, axis):
        length = value.shape[axis]
        return pltpu.roll(value, 1, axis), pltpu.roll(value, length - 1, axis)

    def both(value, axis):
        before, after = shifts(value, axis)
        return before + after

    def stream():
        def planes(x, carry):
            scale = wide[3, x]
            m0, m1, m2 = (scale * grid[c, x] for c in range(3))
            moved[0, x], moved[1, x], moved[2, x] = m0, m1, m2
            before, after = shifts(m0, 0)
            sy0, dy0 = before + after, before - after
            before, after = shifts(m1, 0)
            sy1, dy1 = before + after, before - after
            before, after = shifts(m0, 1)
            sz0, dz0 = before + after, before - after
            before, after = shifts(m2, 1)
            sz2, dz2 = before + after, before - after
            before, after = shifts(dz2, 0)
            dyz2 = before - after
            before, after = shifts(dy1, 1)
            dyz1 = before - after
            plane_a[0, x] = 2.0 * m0 + sy0 + sz0
            plane_b[0, x] = dy1 + dz2
            plane_a[1, x] = sy1
            plane_b[1, x] = dy0
            plane_c[0, x] = 2.0 * sy1 + both(sy1, 1) + dyz2
            plane_a[2, x] = sz2
            plane_b[2, x] = dz0
            plane_c[1, x] = 2.0 * sz2 + both(sz2, 0) + dyz1
            return carry

        lax.fori_loop(0, WX, planes, 0)

        def velocity(x, carry):
            half = wide[3, x] * 0.5
            for c in range(3):
                post = plane_a[c, x - 1] + plane_a[c, x + 1] + plane_b[c, x - 1] - plane_b[c, x + 1]
                if c:
                    post = post + plane_c[c - 1, x]
                high, low = split(half * (moved[c, x] + post * (1.0 / 12.0)))
                vel_h[c, x - 1] = high
                vel_l[c, x - 1] = low
            return carry

        lax.fori_loop(1, 12, velocity, 0)

    def apply(a, carry):
        send_vector(a)

        @pl.when(a == 0)
        def _():
            for g in ORDER:
                for j in range(3):
                    if (g, j) != (CENTRE, 2):
                        build(g, j)

        spread(a)
        stream()
        for c, value in enumerate(interpolate()):
            vector = vecs[a, c : c + 1]
            image = live * (value + stiff * vector)
            images[a, c : c + 1] = image
            vecs[a + 1, c : c + 1] = image - SHIFT * vector
        return carry

    lax.fori_loop(0, ITERS, apply, 0)

    lane_row = lax.broadcasted_iota(jnp.int32, (1, 128), 1)
    v = [vecs[k, 0:3] for k in range(3)]
    w = [images[k, 0:3] for k in range(3)]
    pairs = [(v[i], w[j]) for i in range(3) for j in range(i, 3)] + [(v[0], v[j]) for j in range(3)]
    row = jnp.zeros((1, 128), F32)
    for k, (left, right) in enumerate(pairs):
        row = jnp.where(lane_row == k, jnp.sum(left * right), row)
    me = iy * size_z + iz
    part[...] = row
    recv_a[me] = row

    def send_mate(k, carry):
        remote(part, recv_a.at[me], send_r.at[0], got_r.at[0], mate(k)).start()
        return carry

    lax.fori_loop(1, size_y * size_z, send_mate, 0)
    drain(recv_a.at[0 : size_y * size_z - 1], got_r.at[0])
    total = jnp.sum(recv_a[...], axis=0)
    part_b[...] = total
    recv_b[ix] = total
    for k in range(1, size_x):
        remote(part_b, recv_b.at[ix], send_r.at[1], got_r.at[1], along(k)).start()
    drain(recv_b.at[0 : size_x - 1], got_r.at[1])
    total = jnp.sum(recv_b[...], axis=0)
    h00, h01, h02, h11, h12, h22, b0, b1, b2 = (
        jnp.sum(jnp.where(lane_row == k, total, 0.0), axis=1, keepdims=True) for k in range(9)
    )

    def over(top, pivot, size):
        fine = pivot > 1e-7 * size
        return jnp.where(fine, top / jnp.where(fine, pivot, 1.0), 0.0)

    l10 = over(h01, h00, h00)
    l20 = over(h02, h00, h00)
    d1 = h11 - l10 * h01
    e12 = h12 - l10 * h02
    l21 = over(e12, d1, h11)
    d2 = h22 - l20 * h02 - l21 * e12
    z1 = b1 - l10 * b0
    z2 = b2 - l20 * b0 - l21 * z1
    y2 = over(z2, d2, h22)
    y1 = over(z1, d1, h11) - l21 * y2
    y0 = over(b0, h00, h00) - l10 * y1 - l20 * y2
    out_ref[...] = y0 * v[0] + y1 * v[1] + y2 * v[2]

    for dx, dy in GROUPS:
        if (dx, dy) != (0, 0):
            halo_copy(dx, dy).wait_send()
    drain(recv_z, send_z)
    drain(marks.at[0:26], send_m)
    for a in range(ITERS):
        drain(recv_v.at[a, 0:26], send_v.at[a])
    drain(recv_a.at[0 : size_y * size_z - 1], send_r.at[0])
    drain(recv_b.at[0 : size_x - 1], send_r.at[1])


def solution(mesh):
    sizes = tuple(mesh.shape[a] for a in AXES)
    plane = sizes[1] * sizes[2]

    def body(density, base_velocity, cells, offsets, target, stiffness, counts):
        vmem = pl.BlockSpec(memory_space=pltpu.VMEM)
        return pl.pallas_call(
            functools.partial(kernel, sizes),
            out_shape=jax.ShapeDtypeStruct((3, CAP), F32),
            in_specs=[vmem] * 6 + [pl.BlockSpec(memory_space=pltpu.SMEM)],
            out_specs=vmem,
            scratch_shapes=[
                pltpu.VMEM((4, CX, CY, CZ), F32),
                pltpu.VMEM((CZ, 4 * CX * CY), F32),
                pltpu.VMEM((8, 4 * CX * CY), F32),
                pltpu.VMEM((8, CAP), F32),
                pltpu.VMEM((9, 4, CX, CY, CZ), F32),
                pltpu.VMEM((18, 8, 4 * CX * CY), F32),
                pltpu.VMEM((27, 8, CAP), F32),
                pltpu.VMEM((4, WX, WY, CZ), F32),
                pltpu.VMEM((4, WX, WY, CZ), F32),
                pltpu.VMEM((4, CX, CY, CZ), F32),
                pltpu.VMEM((4, WX, WY, WZ), F32),
                pltpu.VMEM((9, TZ, 3 * CAP), BF16),
                pltpu.VMEM((9, TZ, 3 * CAP), BF16),
                pltpu.VMEM((WZ, CAP), BF16),
                pltpu.VMEM((WZ, CAP), BF16),
                pltpu.VMEM((sum(SPANS), 3 * CAP), F32),
                pltpu.VMEM((3 * max(SPANS), 3 * CAP), BF16),
                pltpu.VMEM((3 * max(SPANS), 3 * CAP), BF16),
                pltpu.VMEM((3, WX, WY, WZ), F32),
                pltpu.VMEM((3, WX, WY, WZ), F32),
                pltpu.VMEM((3, WX, WY, WZ), F32),
                pltpu.VMEM((3, WX, WY, WZ), F32),
                pltpu.VMEM((2, WX, WY, WZ), F32),
                pltpu.VMEM((3, 11, WY, WZ), BF16),
                pltpu.VMEM((3, 11, WY, WZ), BF16),
                pltpu.VMEM((ITERS + 1, 4, CAP), F32),
                pltpu.VMEM((ITERS, 4, CAP), F32),
                pltpu.VMEM((ITERS, 27, 4, CAP), F32),
                pltpu.VMEM((1, 128), F32),
                pltpu.VMEM((plane, 1, 128), F32),
                pltpu.VMEM((1, 128), F32),
                pltpu.VMEM((sizes[0], 1, 128), F32),
                pltpu.SemaphoreType.DMA((9,)),
                pltpu.SemaphoreType.DMA((9,)),
                pltpu.SemaphoreType.DMA,
                pltpu.SemaphoreType.DMA,
                pltpu.SemaphoreType.DMA,
                pltpu.SemaphoreType.DMA,
                pltpu.SemaphoreType.DMA((ITERS,)),
                pltpu.SemaphoreType.DMA((ITERS, 9)),
                pltpu.SemaphoreType.DMA((2,)),
                pltpu.SemaphoreType.DMA((2,)),
            ],
            compiler_params=pltpu.CompilerParams(
                collective_id=0, has_side_effects=True, vmem_limit_bytes=60 * 1024 * 1024
            ),
            name="immersed",
        )(density, base_velocity, cells, offsets, target, stiffness[None], counts)

    return jax.shard_map(
        body,
        mesh=mesh,
        in_specs=(
            P(*AXES), P(None, *AXES), P(None, ALL), P(None, ALL), P(None, ALL), P(ALL), P(ALL),
        ),
        out_specs=P(None, ALL),
        check_vma=False,
    )
```

```python
import functools

import jax
import jax.numpy as jnp
from jax import lax
from jax.experimental import pallas as pl
from jax.experimental.pallas import tpu as pltpu
from jax.sharding import PartitionSpec as P

ITERS = 3
CX, CY, CZ = 8, 8, 128
CAP = 256
WX, WY, WZ = 13, 16, 256
TZ = 144
AXES = ("gx", "gy", "gz")
ALL = ("gx", "gy", "gz")
MESH = pl.DeviceIdType.MESH
SHIFT = 0.1
F32, BF16 = jnp.float32, jnp.bfloat16

GROUPS = [(dx, dy) for dx in (-1, 0, 1) for dy in (-1, 0, 1)]
DZS = (-1, 1, 0)
ORDER = sorted(range(9), key=lambda g: abs(GROUPS[g][0]) + abs(GROUPS[g][1]))
PLANES = {-1: (0, 4), 0: (1, 12), 1: (9, 4)}
ROWS = {-1: (0, 8), 0: (0, 16), 1: (8, 8)}
TAKE = {-1: (6, 8), 0: (0, 8), 1: (0, 3)}


def group_of(dx, dy):
    return (dx + 1) * 3 + dy + 1


def slot_of(dx, dy, dz):
    return group_of(dx, dy) * 3 + DZS.index(dz)


NEIGHBOURS = [
    (GROUPS[g][0], GROUPS[g][1], dz)
    for g in ORDER
    for dz in DZS
    if (GROUPS[g][0], GROUPS[g][1], dz) != (0, 0, 0)
]
CENTRE = group_of(0, 0)
SPANS = [PLANES[dx][1] * ROWS[dy][1] for dx, dy in GROUPS]
STARTS = [sum(SPANS[:g]) for g in range(9)]


def split(value):
    high = value.astype(BF16)
    return high, (value - high.astype(F32)).astype(BF16)


def dot3(lh, ll, rh, rl, dims):
    dot = functools.partial(
        lax.dot_general, dimension_numbers=(dims, ((), ())), preferred_element_type=F32
    )
    return dot(lh, rh) + (dot(ll, rh) + dot(lh, rl))


def kernel(
    sizes,
    density_in, base_in, cells_in, offsets_in, target_in, stiff_in, counts_ref,
    out_ref,
    density_ref, cells_ref, offsets_ref, target_ref, stiff_ref,
    field, ftrans, pack_lo, pack_hi, pack_z_lo, pack_z_hi, mark_own, recv_x, recv_lo, recv_hi,
    recv_z_lo, recv_z_hi, columns, marks, main, halo, ztile, wide,
    table_h, table_l, own_h, own_l, wxy, wxy_h, wxy_l, edge_w, left_h, left_l, grid, edges, moved, plane_a, plane_b, plane_c,
    vel_h, vel_l, energy_ref, vecs, images, recv_v, part, recv_a, part_b, recv_b,
    loaded, send_f, got_f, send_z, got_z, send_m, got_m, send_v, got_v, send_r, got_r,
):
    size_x, size_y, size_z = sizes
    ix, iy, iz = (lax.axis_index(a) for a in AXES)

    def at(dx, dy, dz):
        return (
            lax.rem(ix + dx + size_x, size_x),
            lax.rem(iy + dy + size_y, size_y),
            lax.rem(iz + dz + size_z, size_z),
        )

    def mate(k):
        rest = lax.rem(iy * size_z + iz + k, size_y * size_z)
        return (ix, rest // size_z, lax.rem(rest, size_z))

    def along(k):
        return (lax.rem(ix + k, size_x), iy, iz)

    loads = [
        pltpu.make_async_copy(base_in.at[c], field.at[:, c], loaded.at[c]) for c in range(3)
    ]
    loads += [
        pltpu.make_async_copy(source, target, loaded.at[3 + k])
        for k, (source, target) in enumerate(
            [
                (density_in, density_ref), (cells_in, cells_ref), (offsets_in, offsets_ref),
                (target_in, target_ref), (stiff_in, stiff_ref),
            ]
        )
    ]
    for load in loads:
        load.start()

    barrier = pltpu.get_barrier_semaphore()
    for offset in NEIGHBOURS:
        pl.semaphore_signal(barrier, inc=1, device_id=at(*offset), device_id_type=MESH)

    def greet_mate(k, carry):
        pl.semaphore_signal(barrier, inc=1, device_id=mate(k), device_id_type=MESH)
        return carry

    lax.fori_loop(1, size_y * size_z, greet_mate, 0)
    for k in range(1, size_x):
        pl.semaphore_signal(barrier, inc=1, device_id=along(k), device_id_type=MESH)

    for load in loads:
        load.wait()
    field[:, 3] = lax.rsqrt(density_ref[...])
    ftrans[...] = field[...].reshape(4 * CX * CY, CZ).T
    pack_z_lo[...] = ftrans[CZ - 2 : CZ]
    pack_z_hi[...] = ftrans[0:4]
    for c in range(4):
        pack_lo[:, 2 * c : 2 * c + 2] = field[:, c, CY - 2 : CY]
        pack_hi[:, 4 * c : 4 * c + 4] = field[:, c, 0:4]
    anchors = (ix * CX, iy * CY, iz * CZ)
    for k in range(3):
        mark_own[k : k + 1] = (cells_ref[k : k + 1] - anchors[k]).astype(F32)
    mark_own[3:6] = offsets_ref[...]
    mark_own[6:8] = jnp.zeros((2, CAP), F32)
    marks[slot_of(0, 0, 0)] = mark_own[...]

    pl.semaphore_wait(barrier, len(NEIGHBOURS) + size_y * size_z - 1 + size_x - 1)

    def remote(src, dst, send, recv, device):
        return pltpu.make_async_remote_copy(
            src_ref=src, dst_ref=dst, send_sem=send, recv_sem=recv, device_id=device,
            device_id_type=MESH,
        )

    def drain(ref, sem):
        pltpu.make_async_copy(ref, ref, sem).wait()

    def halo_copy(dx, dy):
        a, b = TAKE[-dx]
        g = group_of(-dx, -dy)
        if dy == 0:
            pair = field.at[a:b], recv_x.at[dx == -1 and 1 or 0, a:b]
        elif dy == 1:
            pair = pack_lo.at[a:b], recv_lo.at[1 - dx, a:b]
        else:
            pair = pack_hi.at[a:b], recv_hi.at[1 - dx, a:b]
        return remote(*pair, send_f.at[g], got_f.at[g], at(dx, dy, 0))

    def edge_copy(dx, dy, dz):
        a, b = {-1: (0, 128), 0: (0, 256), 1: (128, 256)}[dx]
        g = group_of(-dx, -dy)
        if dz == 1:
            pair = pack_z_lo.at[:, a:b], recv_z_lo.at[g, :, a:b]
        else:
            pair = pack_z_hi.at[:, a:b], recv_z_hi.at[g, :, a:b]
        side = (1 - dz) // 2
        return remote(*pair, send_z.at[side], got_z.at[side], at(dx, dy, dz))

    for dx, dy in GROUPS:
        if (dx, dy) != (0, 0):
            halo_copy(dx, dy).start()
    for dx, dy, dz in NEIGHBOURS:
        if dz:
            edge_copy(dx, dy, dz).start()
    for dx, dy, dz in NEIGHBOURS:
        back = slot_of(-dx, -dy, -dz)
        remote(mark_own, marks.at[back], send_m, got_m, at(dx, dy, dz)).start()

    own_h[...] = jnp.zeros(own_h.shape, BF16)
    own_l[...] = jnp.zeros(own_l.shape, BF16)
    ztile[...] = jnp.zeros(ztile.shape, F32)
    columns[...] = jnp.zeros(columns.shape, F32)
    main[:, :, 8:16] = jnp.zeros((WX, 4, 8, CZ), F32)
    halo[:, :, 8:16] = jnp.zeros((WX, 4, 8, CZ), F32)
    grid[...] = jnp.zeros(grid.shape, F32)
    edges[...] = jnp.zeros(edges.shape, F32)
    vecs[...] = jnp.zeros(vecs.shape, F32)

    live = (lax.broadcasted_iota(jnp.int32, (1, CAP), 1) < counts_ref[0]).astype(F32)
    stiff = stiff_ref[...]

    def axis_table(first, rows, start, weights):
        away = (
            lax.broadcasted_iota(jnp.int32, (rows, CAP), 0).astype(F32) + float(first) - start
        )
        value = jnp.zeros((rows, CAP), F32)
        for step in range(4):
            value = jnp.where(away == float(step), weights[step], value)
        return value

    def build(g, j):
        (dx, dy), dz = GROUPS[g], DZS[j]
        mark = marks[g * 3 + j]
        fraction = mark[3:6]
        root = jnp.sqrt(1.0 + 4.0 * fraction - 4.0 * fraction * fraction)
        weights = [
            (3.0 - 2.0 * fraction - root) * 0.125,
            (3.0 - 2.0 * fraction + root) * 0.125,
            (1.0 + 2.0 * fraction + root) * 0.125,
            (1.0 + 2.0 * fraction - root) * 0.125,
        ]
        of = lambda k: [w[k : k + 1] for w in weights]
        x0, nx = PLANES[dx]
        y0, ny = ROWS[dy]
        table_x = axis_table(x0, 16, mark[0:1] + float(1 + CX * dx), of(0))
        table_y = axis_table(y0, ny, mark[1:2] + float(1 + CY * dy), of(1))
        for x in range(nx):
            rows = slice(STARTS[g] + x * ny, STARTS[g] + (x + 1) * ny)
            weight = table_x[x : x + 1] * table_y
            if dz == 0:
                wxy[rows] = weight
            else:
                high, low = split(weight)
                wxy_h[j, rows] = high
                wxy_l[j, rows] = low
        start = mark[2:3] + float(1 + CZ * dz)
        if dz == 0:
            high, low = split(axis_table(0, TZ, start, of(2)))
            table_h[g] = high
            table_l[g] = low
            if g == CENTRE:
                own_h[0:TZ] = high
                own_l[0:TZ] = low
        else:
            touched = axis_table({-1: 0, 1: CZ + 1}[dz], 8, start, of(2))[0:4]
            edge_w[2 * g + j, 0:12] = jnp.concatenate([touched] * 3, axis=0)
            edge_w[2 * g + j, 12:16] = jnp.zeros((4, CAP), F32)

    build(CENTRE, 2)

    for g, (dx, dy) in enumerate(GROUPS):
        if g != CENTRE:
            halo_copy(-dx, -dy).wait_recv()
    drain(recv_z_lo.at[0:6], got_z.at[0])
    drain(recv_z_hi.at[0:6], got_z.at[1])
    for g, (dx, dy) in enumerate(GROUPS):
        (xa, xb), (ya, yb) = TAKE[dx], TAKE[dy]
        x0, y0 = xa + CX * dx + 2, ya + CY * dy + 2
        planes = slice(x0, x0 + xb - xa)
        if g == CENTRE:
            main[planes, :, y0 : y0 + CY] = field[...]
        elif dy == 0:
            main[planes, :, y0 : y0 + CY] = recv_x[dx == 1 and 1 or 0, xa:xb]
        else:
            source, step = (recv_lo, 2) if dy == -1 else (recv_hi, 4)
            for c in range(4):
                main[planes, c, y0 : y0 + yb - ya] = source[
                    dx + 1, xa:xb, c * step : c * step + yb - ya
                ]
        columns[0:2] = recv_z_lo[g]
        columns[2:6] = recv_z_hi[g]
        ztile[:, :, :, 0:8] = columns[...].T.reshape(CX, 4, CY, 8)
        halo[planes, :, y0 : y0 + yb - ya] = ztile[xa:xb, :, ya:yb]
    lane = lax.broadcasted_iota(jnp.int32, (WY, CZ), 1)

    for x in range(WX):
        for c in range(4):
            turned = pltpu.roll(main[x, c], 2, 1)
            edge = halo[x, c]
            wide[c, x, :, 0:CZ] = jnp.where(lane < 2, edge, turned)
            wide[c, x, :, CZ:] = jnp.where(lane < 2, turned, jnp.where(lane < 5, edge, 0.0))

    def interpolate():
        high = vel_h[...].reshape(3 * 11 * WY, WZ)
        low = vel_l[...].reshape(3 * 11 * WY, WZ)
        rows = dot3(high, low, own_h[...], own_l[...], ((1,), (0,)))
        weight = wxy[STARTS[CENTRE] : STARTS[CENTRE] + 11 * WY]
        return [
            jnp.sum(rows[c * 11 * WY : (c + 1) * 11 * WY] * weight, axis=0, keepdims=True)
            for c in range(3)
        ]

    for c in range(3):
        high, low = split(wide[c, 1:12])
        vel_h[c] = high
        vel_l[c] = low
    for c, value in enumerate(interpolate()):
        vecs[0, c : c + 1] = live * (target_ref[c : c + 1] - value)

    drain(marks.at[0:26], got_m)

    def send_vector(a):
        for dx, dy, dz in NEIGHBOURS:
            back = slot_of(-dx, -dy, -dz)
            remote(
                vecs.at[a], recv_v.at[a, back], send_v.at[a], got_v.at[a, back // 3], at(dx, dy, dz)
            ).start()
        recv_v[a, slot_of(0, 0, 0)] = vecs[a]

    part_row = lax.broadcasted_iota(jnp.int32, (16, CAP), 0)

    def spread_inner(a, g):
        span = SPANS[g]
        vector = recv_v[a, 3 * g + 2]
        weight = wxy[STARTS[g] : STARTS[g] + span]
        for c in range(3):
            high, low = split(weight * vector[c : c + 1])
            left_h[c * span : (c + 1) * span] = high
            left_l[c * span : (c + 1) * span] = low
        return dot3(left_h[0 : 3 * span], left_l[0 : 3 * span], table_h[g], table_l[g], ((1,), (1,)))

    def spread_edges(a, g):
        rows = slice(STARTS[g], STARTS[g] + SPANS[g])
        sides = []
        for j in range(2):
            vector = recv_v[a, 3 * g + j]
            value = jnp.where(
                part_row < 4, vector[0:1], jnp.where(part_row < 8, vector[1:2], vector[2:3])
            )
            high, low = split(edge_w[2 * g + j] * value)
            sides.append(dot3(high, low, wxy_h[j, rows], wxy_l[j, rows], ((1,), (1,))))
        return jnp.concatenate(sides, axis=0).T

    def spread(a):
        grid[:, :, :, 0:TZ] = jnp.zeros((3, WX, WY, TZ), F32)
        edges[:, :, 0:32] = jnp.zeros((WX, WY, 32), F32)
        for g in ORDER:
            (dx, dy) = GROUPS[g]
            span = SPANS[g]
            x0, nx = PLANES[dx]
            y0, ny = ROWS[dy]
            if g == CENTRE:
                total = spread_inner(a, g)
                drain(recv_v.at[a, 3 * g : 3 * g + 2], got_v.at[a, g])
            else:
                drain(recv_v.at[a, 3 * g : 3 * g + 3], got_v.at[a, g])
                total = spread_inner(a, g)
            for c in range(3):
                at_place = (c, slice(x0, x0 + nx), slice(y0, y0 + ny), slice(0, TZ))
                grid[at_place] += total[c * span : (c + 1) * span].reshape(nx, ny, TZ)
            edges[x0 : x0 + nx, y0 : y0 + ny, 0:32] += spread_edges(a, g).reshape(nx, ny, 32)

    def shifts(value, axis):
        length = value.shape[axis]
        return pltpu.roll(value, 1, axis), pltpu.roll(value, length - 1, axis)

    def both(value, axis):
        before, after = shifts(value, axis)
        return before + after

    def stream():
        for x in range(WX):
            scale = wide[3, x]
            edge = edges[x]
            values = []
            for c in range(3):
                head = grid[c, x, :, 0:CZ] + jnp.where(
                    lane < 4, pltpu.roll(edge, CZ - 4 * c, 1) if c else edge, 0.0
                )
                tail = grid[c, x, :, CZ:] + jnp.where(
                    (lane > 0) & (lane < 5), pltpu.roll(edge, CZ - 15 - 4 * c, 1), 0.0
                )
                values.append(scale * jnp.concatenate([head, tail], axis=1))
            m0, m1, m2 = values
            moved[0, x], moved[1, x], moved[2, x] = m0, m1, m2
            before, after = shifts(m0, 0)
            sy0, dy0 = before + after, before - after
            before, after = shifts(m1, 0)
            sy1, dy1 = before + after, before - after
            before, after = shifts(m0, 1)
            sz0, dz0 = before + after, before - after
            before, after = shifts(m2, 1)
            sz2, dz2 = before + after, before - after
            before, after = shifts(dz2, 0)
            dyz2 = before - after
            before, after = shifts(dy1, 1)
            dyz1 = before - after
            plane_a[0, x] = 2.0 * m0 + sy0 + sz0
            plane_b[0, x] = dy1 + dz2
            plane_a[1, x] = sy1
            plane_b[1, x] = dy0
            plane_c[0, x] = 2.0 * sy1 + both(sy1, 1) + dyz2
            plane_a[2, x] = sz2
            plane_b[2, x] = dz0
            plane_c[1, x] = 2.0 * sz2 + both(sz2, 0) + dyz1

        energy = jnp.zeros((WY, WZ), F32)
        for x in range(1, 12):
            half = wide[3, x] * 0.5
            for c in range(3):
                post = plane_a[c, x - 1] + plane_a[c, x + 1] + plane_b[c, x - 1] - plane_b[c, x + 1]
                if c:
                    post = post + plane_c[c - 1, x]
                response = moved[c, x] + post * (1.0 / 12.0)
                high, low = split(half * response)
                vel_h[c, x - 1] = high
                vel_l[c, x - 1] = low
                if 2 <= x < 2 + CX:
                    energy = energy + moved[c, x] * response
        energy_ref[...] = energy

    def apply(a, carry):
        send_vector(a)

        @pl.when(a == 0)
        def _():
            for g in ORDER:
                for j in range(3):
                    if (g, j) != (CENTRE, 2):
                        build(g, j)

        spread(a)
        stream()

        @pl.when(a < ITERS - 1)
        def _():
            for c, value in enumerate(interpolate()):
                vector = vecs[a, c : c + 1]
                image = live * (value + stiff * vector)
                images[a, c : c + 1] = image
                vecs[a + 1, c : c + 1] = image - SHIFT * vector

        return carry

    lax.fori_loop(0, ITERS, apply, 0)

    lane_row = lax.broadcasted_iota(jnp.int32, (1, 128), 1)
    v = [vecs[k, 0:3] for k in range(3)]
    w = [images[k, 0:3] for k in range(2)]
    inside = lambda axis, size: (
        lax.broadcasted_iota(jnp.int32, (WY, WZ), axis) - 2
    ).astype(jnp.uint32) < size
    energy = jnp.where(inside(0, CY) & inside(1, CZ), energy_ref[...], 0.0)
    last = 0.5 * jnp.sum(energy) + jnp.sum(stiff * v[2] * v[2])
    pairs = [(v[0], w[0]), (v[0], w[1]), (v[2], w[0]), (v[1], w[1]), (v[2], w[1])]
    pairs = pairs + [(v[0], v[j]) for j in range(3)]
    row = jnp.zeros((1, 128), F32)
    for k, (left, right) in enumerate(pairs):
        row = jnp.where(lane_row == k, jnp.sum(left * right), row)
    row = jnp.where(lane_row == len(pairs), last, row)
    me = iy * size_z + iz
    part[...] = row
    recv_a[me] = row

    def send_mate(k, carry):
        remote(part, recv_a.at[me], send_r.at[0], got_r.at[0], mate(k)).start()
        return carry

    lax.fori_loop(1, size_y * size_z, send_mate, 0)
    drain(recv_a.at[0 : size_y * size_z - 1], got_r.at[0])
    total = jnp.sum(recv_a[...], axis=0)
    part_b[...] = total
    recv_b[ix] = total
    for k in range(1, size_x):
        remote(part_b, recv_b.at[ix], send_r.at[1], got_r.at[1], along(k)).start()
    drain(recv_b.at[0 : size_x - 1], got_r.at[1])
    total = jnp.sum(recv_b[...], axis=0)
    h00, h01, h02, h11, h12, b0, b1, b2, h22 = (
        jnp.sum(jnp.where(lane_row == k, total, 0.0), axis=1, keepdims=True) for k in range(9)
    )

    def over(top, pivot, size):
        fine = pivot > 1e-7 * size
        return jnp.where(fine, top / jnp.where(fine, pivot, 1.0), 0.0)

    l10 = over(h01, h00, h00)
    l20 = over(h02, h00, h00)
    d1 = h11 - l10 * h01
    e12 = h12 - l10 * h02
    l21 = over(e12, d1, h11)
    d2 = h22 - l20 * h02 - l21 * e12
    z1 = b1 - l10 * b0
    z2 = b2 - l20 * b0 - l21 * z1
    y2 = over(z2, d2, h22)
    y1 = over(z1, d1, h11) - l21 * y2
    y0 = over(b0, h00, h00) - l10 * y1 - l20 * y2
    out_ref[...] = y0 * v[0] + y1 * v[1] + y2 * v[2]

    for dx, dy in GROUPS:
        if (dx, dy) != (0, 0):
            halo_copy(dx, dy).wait_send()
    drain(recv_z_lo.at[0:6], send_z.at[0])
    drain(recv_z_hi.at[0:6], send_z.at[1])
    drain(marks.at[0:26], send_m)
    for a in range(ITERS):
        drain(recv_v.at[a, 0:26], send_v.at[a])
    drain(recv_a.at[0 : size_y * size_z - 1], send_r.at[0])
    drain(recv_b.at[0 : size_x - 1], send_r.at[1])


def solution(mesh):
    sizes = tuple(mesh.shape[a] for a in AXES)
    plane = sizes[1] * sizes[2]

    def body(density, base_velocity, cells, offsets, target, stiffness, counts):
        vmem = pl.BlockSpec(memory_space=pltpu.VMEM)
        return pl.pallas_call(
            functools.partial(kernel, sizes),
            out_shape=jax.ShapeDtypeStruct((3, CAP), F32),
            in_specs=[pl.BlockSpec(memory_space=pl.ANY)] * 6 + [pl.BlockSpec(memory_space=pltpu.SMEM)],
            out_specs=vmem,
            scratch_shapes=[
                pltpu.VMEM((CX, CY, CZ), F32),
                pltpu.VMEM((3, CAP), jnp.int32),
                pltpu.VMEM((3, CAP), F32),
                pltpu.VMEM((3, CAP), F32),
                pltpu.VMEM((1, CAP), F32),
                pltpu.VMEM((CX, 4, CY, CZ), F32),
                pltpu.VMEM((CZ, 4 * CX * CY), F32),
                pltpu.VMEM((CX, 8, CZ), F32),
                pltpu.VMEM((CX, 16, CZ), F32),
                pltpu.VMEM((2, 4 * CX * CY), F32),
                pltpu.VMEM((4, 4 * CX * CY), F32),
                pltpu.VMEM((8, CAP), F32),
                pltpu.VMEM((2, CX, 4, CY, CZ), F32),
                pltpu.VMEM((3, CX, 8, CZ), F32),
                pltpu.VMEM((3, CX, 16, CZ), F32),
                pltpu.VMEM((9, 2, 4 * CX * CY), F32),
                pltpu.VMEM((9, 4, 4 * CX * CY), F32),
                pltpu.VMEM((8, 4 * CX * CY), F32),
                pltpu.VMEM((27, 8, CAP), F32),
                pltpu.VMEM((WX, 4, WY, CZ), F32),
                pltpu.VMEM((WX, 4, WY, CZ), F32),
                pltpu.VMEM((CX, 4, CY, CZ), F32),
                pltpu.VMEM((4, WX, WY, WZ), F32),
                pltpu.VMEM((9, TZ, CAP), BF16),
                pltpu.VMEM((9, TZ, CAP), BF16),
                pltpu.VMEM((WZ, CAP), BF16),
                pltpu.VMEM((WZ, CAP), BF16),
                pltpu.VMEM((sum(SPANS), CAP), F32),
                pltpu.VMEM((2, sum(SPANS), CAP), BF16),
                pltpu.VMEM((2, sum(SPANS), CAP), BF16),
                pltpu.VMEM((18, 16, CAP), F32),
                pltpu.VMEM((3 * max(SPANS), CAP), BF16),
                pltpu.VMEM((3 * max(SPANS), CAP), BF16),
                pltpu.VMEM((3, WX, WY, WZ), F32),
                pltpu.VMEM((WX, WY, CZ), F32),
                pltpu.VMEM((3, WX, WY, WZ), F32),
                pltpu.VMEM((3, WX, WY, WZ), F32),
                pltpu.VMEM((3, WX, WY, WZ), F32),
                pltpu.VMEM((2, WX, WY, WZ), F32),
                pltpu.VMEM((3, 11, WY, WZ), BF16),
                pltpu.VMEM((3, 11, WY, WZ), BF16),
                pltpu.VMEM((WY, WZ), F32),
                pltpu.VMEM((ITERS + 1, 4, CAP), F32),
                pltpu.VMEM((ITERS, 4, CAP), F32),
                pltpu.VMEM((ITERS, 27, 4, CAP), F32),
                pltpu.VMEM((1, 128), F32),
                pltpu.VMEM((plane, 1, 128), F32),
                pltpu.VMEM((1, 128), F32),
                pltpu.VMEM((sizes[0], 1, 128), F32),
                pltpu.SemaphoreType.DMA((8,)),
                pltpu.SemaphoreType.DMA((9,)),
                pltpu.SemaphoreType.DMA((9,)),
                pltpu.SemaphoreType.DMA((2,)),
                pltpu.SemaphoreType.DMA((2,)),
                pltpu.SemaphoreType.DMA,
                pltpu.SemaphoreType.DMA,
                pltpu.SemaphoreType.DMA((ITERS,)),
                pltpu.SemaphoreType.DMA((ITERS, 9)),
                pltpu.SemaphoreType.DMA((2,)),
                pltpu.SemaphoreType.DMA((2,)),
            ],
            compiler_params=pltpu.CompilerParams(
                collective_id=0, has_side_effects=True, vmem_limit_bytes=60 * 1024 * 1024
            ),
            name="immersed",
        )(density, base_velocity, cells, offsets, target, stiffness[None], counts)

    return jax.shard_map(
        body,
        mesh=mesh,
        in_specs=(
            P(*AXES), P(None, *AXES), P(None, ALL), P(None, ALL), P(None, ALL), P(ALL), P(ALL),
        ),
        out_specs=P(None, ALL),
        check_vma=False,
    )
```

```python
import functools

import jax
import jax.numpy as jnp
from jax import lax
from jax.experimental import pallas as pl
from jax.experimental.pallas import tpu as pltpu
from jax.sharding import PartitionSpec as P

ITERS = 3
CX, CY, CZ = 8, 8, 128
CAP = 256
WX, WY, WZ = 13, 16, 256
TZ = 144
AXES = ("gx", "gy", "gz")
ALL = ("gx", "gy", "gz")
MESH = pl.DeviceIdType.MESH
SHIFT = 0.1
F32, BF16 = jnp.float32, jnp.bfloat16

GROUPS = [(dx, dy) for dx in (-1, 0, 1) for dy in (-1, 0, 1)]
DZS = (-1, 1, 0)
ORDER = sorted(range(9), key=lambda g: abs(GROUPS[g][0]) + abs(GROUPS[g][1]))
PLANES = {-1: (0, 4), 0: (1, 12), 1: (9, 4)}
ROWS = {-1: (0, 8), 0: (0, 16), 1: (8, 8)}
TAKE = {-1: (6, 8), 0: (0, 8), 1: (0, 3)}


def group_of(dx, dy):
    return (dx + 1) * 3 + dy + 1


def slot_of(dx, dy, dz):
    return group_of(dx, dy) * 3 + DZS.index(dz)


NEIGHBOURS = [
    (GROUPS[g][0], GROUPS[g][1], dz)
    for g in ORDER
    for dz in DZS
    if (GROUPS[g][0], GROUPS[g][1], dz) != (0, 0, 0)
]
CENTRE = group_of(0, 0)
SPANS = [PLANES[dx][1] * ROWS[dy][1] for dx, dy in GROUPS]
STARTS = [sum(SPANS[:g]) for g in range(9)]


def split(value):
    high = value.astype(BF16)
    return high, (value - high.astype(F32)).astype(BF16)


def dot3(lh, ll, rh, rl, dims):
    dot = functools.partial(
        lax.dot_general, dimension_numbers=(dims, ((), ())), preferred_element_type=F32
    )
    return dot(lh, rh) + (dot(ll, rh) + dot(lh, rl))


def kernel(
    sizes,
    density_in, base_in, cells_in, offsets_in, target_in, stiff_in, counts_in,
    out_ref,
    counts_ref,
    density_ref, cells_ref, offsets_ref, target_ref, stiff_ref,
    field, ftrans, pack_lo, pack_hi, pack_z_lo, pack_z_hi, mark_own, recv_x, recv_lo, recv_hi,
    recv_z_lo, recv_z_hi, columns, marks, main, halo, ztile, wide,
    table_h, table_l, own_h, own_l, wxy, wxy_h, wxy_l, edge_w, left_h, left_l, grid, edges, moved, plane_a, plane_b, plane_c,
    vel_h, vel_l, vecs, images, recv_v, part, recv_a, part_b, recv_b,
    loaded, send_f, got_f, send_z, got_z, send_m, got_m, send_v, got_v, send_r, got_r,
):
    size_x, size_y, size_z = sizes
    ix, iy, iz = (lax.axis_index(a) for a in AXES)

    def at(dx, dy, dz):
        return (
            lax.rem(ix + dx + size_x, size_x),
            lax.rem(iy + dy + size_y, size_y),
            lax.rem(iz + dz + size_z, size_z),
        )

    def mate(k):
        rest = lax.rem(iy * size_z + iz + k, size_y * size_z)
        return (ix, rest // size_z, lax.rem(rest, size_z))

    def along(k):
        return (lax.rem(ix + k, size_x), iy, iz)

    loads = [
        pltpu.make_async_copy(base_in.at[c], field.at[:, c], loaded.at[c]) for c in range(3)
    ]
    loads += [
        pltpu.make_async_copy(source, target, loaded.at[3 + k])
        for k, (source, target) in enumerate(
            [
                (density_in, density_ref), (cells_in, cells_ref), (offsets_in, offsets_ref),
                (target_in, target_ref), (stiff_in, stiff_ref), (counts_in, counts_ref),
            ]
        )
    ]
    for load in loads:
        load.start()

    barrier = pltpu.get_barrier_semaphore()
    for offset in NEIGHBOURS:
        pl.semaphore_signal(barrier, inc=1, device_id=at(*offset), device_id_type=MESH)

    def greet_mate(k, carry):
        pl.semaphore_signal(barrier, inc=1, device_id=mate(k), device_id_type=MESH)
        return carry

    lax.fori_loop(1, size_y * size_z, greet_mate, 0)
    for k in range(1, size_x):
        pl.semaphore_signal(barrier, inc=1, device_id=along(k), device_id_type=MESH)

    for load in loads:
        load.wait()
    field[:, 3] = lax.rsqrt(density_ref[...])
    ftrans[...] = field[...].reshape(4 * CX * CY, CZ).T
    pack_z_lo[...] = ftrans[CZ - 2 : CZ]
    pack_z_hi[...] = ftrans[0:4]
    for c in range(4):
        pack_lo[:, 2 * c : 2 * c + 2] = field[:, c, CY - 2 : CY]
        pack_hi[:, 4 * c : 4 * c + 4] = field[:, c, 0:4]
    anchors = (ix * CX, iy * CY, iz * CZ)
    for k in range(3):
        mark_own[k : k + 1] = (cells_ref[k : k + 1] - anchors[k]).astype(F32)
    mark_own[3:6] = offsets_ref[...]
    mark_own[6:8] = jnp.zeros((2, CAP), F32)
    marks[slot_of(0, 0, 0)] = mark_own[...]

    pl.semaphore_wait(barrier, len(NEIGHBOURS) + size_y * size_z - 1 + size_x - 1)

    def remote(src, dst, send, recv, device):
        return pltpu.make_async_remote_copy(
            src_ref=src, dst_ref=dst, send_sem=send, recv_sem=recv, device_id=device,
            device_id_type=MESH,
        )

    def drain(ref, sem):
        pltpu.make_async_copy(ref, ref, sem).wait()

    def halo_copy(dx, dy):
        a, b = TAKE[-dx]
        g = group_of(-dx, -dy)
        if dy == 0:
            pair = field.at[a:b], recv_x.at[dx == -1 and 1 or 0, a:b]
        elif dy == 1:
            pair = pack_lo.at[a:b], recv_lo.at[1 - dx, a:b]
        else:
            pair = pack_hi.at[a:b], recv_hi.at[1 - dx, a:b]
        return remote(*pair, send_f.at[g], got_f.at[g], at(dx, dy, 0))

    def edge_copy(dx, dy, dz):
        a, b = {-1: (0, 128), 0: (0, 256), 1: (128, 256)}[dx]
        g = group_of(-dx, -dy)
        if dz == 1:
            pair = pack_z_lo.at[:, a:b], recv_z_lo.at[g, :, a:b]
        else:
            pair = pack_z_hi.at[:, a:b], recv_z_hi.at[g, :, a:b]
        side = (1 - dz) // 2
        return remote(*pair, send_z.at[side], got_z.at[side], at(dx, dy, dz))

    for dx, dy in GROUPS:
        if (dx, dy) != (0, 0):
            halo_copy(dx, dy).start()
    for dx, dy, dz in NEIGHBOURS:
        if dz:
            edge_copy(dx, dy, dz).start()
    for dx, dy, dz in NEIGHBOURS:
        back = slot_of(-dx, -dy, -dz)
        remote(mark_own, marks.at[back], send_m, got_m, at(dx, dy, dz)).start()

    own_h[...] = jnp.zeros(own_h.shape, BF16)
    own_l[...] = jnp.zeros(own_l.shape, BF16)
    ztile[...] = jnp.zeros(ztile.shape, F32)
    columns[...] = jnp.zeros(columns.shape, F32)
    main[:, :, 8:16] = jnp.zeros((WX, 4, 8, CZ), F32)
    halo[:, :, 8:16] = jnp.zeros((WX, 4, 8, CZ), F32)
    grid[...] = jnp.zeros(grid.shape, F32)
    edges[...] = jnp.zeros(edges.shape, F32)
    vecs[...] = jnp.zeros(vecs.shape, F32)

    live = (lax.broadcasted_iota(jnp.int32, (1, CAP), 1) < counts_ref[0]).astype(F32)
    stiff = stiff_ref[...]

    def axis_table(first, rows, start, weights):
        away = (
            lax.broadcasted_iota(jnp.int32, (rows, CAP), 0).astype(F32) + float(first) - start
        )
        value = jnp.zeros((rows, CAP), F32)
        for step in range(4):
            value = jnp.where(away == float(step), weights[step], value)
        return value

    def build(g, j):
        (dx, dy), dz = GROUPS[g], DZS[j]
        mark = marks[g * 3 + j]
        fraction = mark[3:6]
        root = jnp.sqrt(1.0 + 4.0 * fraction - 4.0 * fraction * fraction)
        weights = [
            (3.0 - 2.0 * fraction - root) * 0.125,
            (3.0 - 2.0 * fraction + root) * 0.125,
            (1.0 + 2.0 * fraction + root) * 0.125,
            (1.0 + 2.0 * fraction - root) * 0.125,
        ]
        of = lambda k: [w[k : k + 1] for w in weights]
        x0, nx = PLANES[dx]
        y0, ny = ROWS[dy]
        table_x = axis_table(x0, 16, mark[0:1] + float(1 + CX * dx), of(0))
        table_y = axis_table(y0, ny, mark[1:2] + float(1 + CY * dy), of(1))
        for x in range(nx):
            rows = slice(STARTS[g] + x * ny, STARTS[g] + (x + 1) * ny)
            weight = table_x[x : x + 1] * table_y
            if dz == 0:
                wxy[rows] = weight
            else:
                high, low = split(weight)
                wxy_h[j, rows] = high
                wxy_l[j, rows] = low
        start = mark[2:3] + float(1 + CZ * dz)
        if dz == 0:
            high, low = split(axis_table(0, TZ, start, of(2)))
            table_h[g] = high
            table_l[g] = low
            if g == CENTRE:
                own_h[0:TZ] = high
                own_l[0:TZ] = low
        else:
            touched = axis_table({-1: 0, 1: CZ + 1}[dz], 8, start, of(2))[0:4]
            edge_w[2 * g + j, 0:12] = jnp.concatenate([touched] * 3, axis=0)
            edge_w[2 * g + j, 12:16] = jnp.zeros((4, CAP), F32)

    build(CENTRE, 2)

    for g, (dx, dy) in enumerate(GROUPS):
        if g != CENTRE:
            halo_copy(-dx, -dy).wait_recv()
    drain(recv_z_lo.at[0:6], got_z.at[0])
    drain(recv_z_hi.at[0:6], got_z.at[1])
    for g, (dx, dy) in enumerate(GROUPS):
        (xa, xb), (ya, yb) = TAKE[dx], TAKE[dy]
        x0, y0 = xa + CX * dx + 2, ya + CY * dy + 2
        planes = slice(x0, x0 + xb - xa)
        if g == CENTRE:
            main[planes, :, y0 : y0 + CY] = field[...]
        elif dy == 0:
            main[planes, :, y0 : y0 + CY] = recv_x[dx == 1 and 1 or 0, xa:xb]
        else:
            source, step = (recv_lo, 2) if dy == -1 else (recv_hi, 4)
            for c in range(4):
                main[planes, c, y0 : y0 + yb - ya] = source[
                    dx + 1, xa:xb, c * step : c * step + yb - ya
                ]
        columns[0:2] = recv_z_lo[g]
        columns[2:6] = recv_z_hi[g]
        ztile[:, :, :, 0:8] = columns[...].T.reshape(CX, 4, CY, 8)
        halo[planes, :, y0 : y0 + yb - ya] = ztile[xa:xb, :, ya:yb]
    lane = lax.broadcasted_iota(jnp.int32, (WY, CZ), 1)

    for x in range(WX):
        for c in range(4):
            turned = pltpu.roll(main[x, c], 2, 1)
            edge = halo[x, c]
            wide[c, x, :, 0:CZ] = jnp.where(lane < 2, edge, turned)
            wide[c, x, :, CZ:] = jnp.where(lane < 2, turned, jnp.where(lane < 5, edge, 0.0))

    def interpolate():
        high = vel_h[...].reshape(3 * 11 * WY, WZ)
        low = vel_l[...].reshape(3 * 11 * WY, WZ)
        rows = dot3(high, low, own_h[...], own_l[...], ((1,), (0,)))
        weight = wxy[STARTS[CENTRE] : STARTS[CENTRE] + 11 * WY]
        return [
            jnp.sum(rows[c * 11 * WY : (c + 1) * 11 * WY] * weight, axis=0, keepdims=True)
            for c in range(3)
        ]

    for c in range(3):
        high, low = split(wide[c, 1:12])
        vel_h[c] = high
        vel_l[c] = low
    for c, value in enumerate(interpolate()):
        vecs[0, c : c + 1] = live * (target_ref[c : c + 1] - value)

    def send_vector(a):
        for dx, dy, dz in NEIGHBOURS:
            back = slot_of(-dx, -dy, -dz)
            remote(
                vecs.at[a], recv_v.at[a, back], send_v.at[a], got_v.at[a, abs(dx) + abs(dy) + abs(dz) - 1],
                at(dx, dy, dz),
            ).start()
        recv_v[a, slot_of(0, 0, 0)] = vecs[a]

    part_row = lax.broadcasted_iota(jnp.int32, (16, CAP), 0)

    def spread_inner(a, g):
        span = SPANS[g]
        vector = recv_v[a, 3 * g + 2]
        weight = wxy[STARTS[g] : STARTS[g] + span]
        for c in range(3):
            high, low = split(weight * vector[c : c + 1])
            left_h[c * span : (c + 1) * span] = high
            left_l[c * span : (c + 1) * span] = low
        return dot3(left_h[0 : 3 * span], left_l[0 : 3 * span], table_h[g], table_l[g], ((1,), (1,)))

    def spread_edges(a, g):
        rows = slice(STARTS[g], STARTS[g] + SPANS[g])
        sides = []
        for j in range(2):
            vector = recv_v[a, 3 * g + j]
            value = jnp.where(
                part_row < 4, vector[0:1], jnp.where(part_row < 8, vector[1:2], vector[2:3])
            )
            high, low = split(edge_w[2 * g + j] * value)
            sides.append(dot3(high, low, wxy_h[j, rows], wxy_l[j, rows], ((1,), (1,))))
        return jnp.concatenate(sides, axis=0).T

    def add_inner(a, g):
        (dx, dy), span = GROUPS[g], SPANS[g]
        x0, nx = PLANES[dx]
        y0, ny = ROWS[dy]
        total = spread_inner(a, g)
        for c in range(3):
            at_place = (c, slice(x0, x0 + nx), slice(y0, y0 + ny), slice(0, TZ))
            grid[at_place] += total[c * span : (c + 1) * span].reshape(nx, ny, TZ)

    def add_edges(a, g):
        dx, dy = GROUPS[g]
        x0, nx = PLANES[dx]
        y0, ny = ROWS[dy]
        edges[x0 : x0 + nx, y0 : y0 + ny, 0:32] += spread_edges(a, g).reshape(nx, ny, 32)

    def spread(a):
        far = [abs(dx) + abs(dy) for dx, dy in GROUPS]
        grid[:, :, :, 0:TZ] = jnp.zeros((3, WX, WY, TZ), F32)
        edges[:, :, 0:32] = jnp.zeros((WX, WY, 32), F32)
        for hops, messages in enumerate((0, 6, 12, 8)):
            if hops:
                drain(recv_v.at[a, 0:messages], got_v.at[a, hops - 1])
            for g in range(9):
                if far[g] == hops:
                    add_inner(a, g)
            for g in range(9):
                if far[g] == hops - 1:
                    add_edges(a, g)

    def shifts(value, axis):
        length = value.shape[axis]
        return pltpu.roll(value, 1, axis), pltpu.roll(value, length - 1, axis)

    def both(value, axis):
        before, after = shifts(value, axis)
        return before + after

    def stream(last):
        for x in range(1, 11) if last else range(WX):
            scale = wide[3, x]
            edge = edges[x]
            values = []
            for c in range(3):
                head = grid[c, x, :, 0:CZ] + jnp.where(
                    lane < 4, pltpu.roll(edge, CZ - 4 * c, 1) if c else edge, 0.0
                )
                tail = grid[c, x, :, CZ:] + jnp.where(
                    (lane > 0) & (lane < 5), pltpu.roll(edge, CZ - 15 - 4 * c, 1), 0.0
                )
                values.append(scale * jnp.concatenate([head, tail], axis=1))
            m0, m1, m2 = values
            moved[0, x], moved[1, x], moved[2, x] = m0, m1, m2
            before, after = shifts(m0, 0)
            sy0, dy0 = before + after, before - after
            before, after = shifts(m1, 0)
            sy1, dy1 = before + after, before - after
            before, after = shifts(m0, 1)
            sz0, dz0 = before + after, before - after
            before, after = shifts(m2, 1)
            sz2, dz2 = before + after, before - after
            before, after = shifts(dz2, 0)
            dyz2 = before - after
            before, after = shifts(dy1, 1)
            dyz1 = before - after
            plane_a[0, x] = 2.0 * m0 + sy0 + sz0
            plane_b[0, x] = dy1 + dz2
            plane_a[1, x] = sy1
            plane_b[1, x] = dy0
            plane_c[0, x] = 2.0 * sy1 + both(sy1, 1) + dyz2
            plane_a[2, x] = sz2
            plane_b[2, x] = dz0
            plane_c[1, x] = 2.0 * sz2 + both(sz2, 0) + dyz1

        energy = jnp.zeros((WY, WZ), F32)
        for x in range(2, 10) if last else range(1, 12):
            half = wide[3, x] * 0.5
            for c in range(3):
                post = plane_a[c, x - 1] + plane_a[c, x + 1] + plane_b[c, x - 1] - plane_b[c, x + 1]
                if c:
                    post = post + plane_c[c - 1, x]
                response = moved[c, x] + post * (1.0 / 12.0)
                if last:
                    energy = energy + moved[c, x] * response
                else:
                    high, low = split(half * response)
                    vel_h[c, x - 1] = high
                    vel_l[c, x - 1] = low
        return energy

    lane_row = lax.broadcasted_iota(jnp.int32, (1, 128), 1)
    me = iy * size_z + iz
    mates = size_y * size_z - 1

    def sum_plane(k, row):
        part[k] = row
        recv_a[k, me] = row
        for other in range(1, mates + 1):
            remote(part.at[k], recv_a.at[k, me], send_r.at[k], got_r.at[k], mate(other)).start()

    def sum_along(k):
        drain(recv_a.at[k, 0:mates], got_r.at[k])
        row = jnp.sum(recv_a[k], axis=0)
        part_b[k] = row
        recv_b[k, ix] = row
        for other in range(1, size_x):
            remote(
                part_b.at[k], recv_b.at[k, ix], send_r.at[2 + k], got_r.at[2 + k], along(other)
            ).start()

    def summed(k):
        drain(recv_b.at[k, 0 : size_x - 1], got_r.at[2 + k])
        return jnp.sum(recv_b[k], axis=0)

    for a in range(ITERS):
        send_vector(a)
        if a == 0:
            drain(marks.at[0:26], got_m)
            for g in ORDER:
                for j in range(3):
                    if (g, j) != (CENTRE, 2):
                        build(g, j)
        last = a == ITERS - 1
        if last:
            v = [vecs[k, 0:3] for k in range(3)]
            w = [images[k, 0:3] for k in range(2)]
            pairs = [(v[0], w[0]), (v[0], w[1]), (v[2], w[0]), (v[1], w[1]), (v[2], w[1])]
            pairs = pairs + [(v[0], v[j]) for j in range(3)]
            row = jnp.zeros((1, 128), F32)
            for k, (left, right) in enumerate(pairs):
                row = jnp.where(lane_row == k, jnp.sum(left * right), row)
            sum_plane(0, row)
        spread(a)
        if last:
            sum_along(0)
        energy = stream(last)
        if not last:
            for c, value in enumerate(interpolate()):
                vector = vecs[a, c : c + 1]
                image = live * (value + stiff * vector)
                images[a, c : c + 1] = image
                vecs[a + 1, c : c + 1] = image - SHIFT * vector

    inside = lambda axis, size: (
        lax.broadcasted_iota(jnp.int32, (WY, WZ), axis) - 2
    ).astype(jnp.uint32) < size
    energy = jnp.where(inside(0, CY) & inside(1, CZ), energy, 0.0)
    own = jnp.sum(0.5 * energy, axis=0, keepdims=True)
    own = own + jnp.sum(stiff * v[2] * v[2], axis=0, keepdims=True)
    sum_plane(1, own[:, 0:128] + own[:, 128:256])
    total = summed(0)
    h00, h01, h02, h11, h12, b0, b1, b2 = (
        jnp.sum(jnp.where(lane_row == k, total, 0.0), axis=1, keepdims=True) for k in range(8)
    )

    def over(top, pivot, size):
        fine = pivot > 1e-7 * size
        return jnp.where(fine, top / jnp.where(fine, pivot, 1.0), 0.0)

    l10 = over(h01, h00, h00)
    l20 = over(h02, h00, h00)
    d1 = h11 - l10 * h01
    e12 = h12 - l10 * h02
    l21 = over(e12, d1, h11)
    less = h02 * l20 + l21 * e12
    z1 = b1 - l10 * b0
    z2 = b2 - l20 * b0 - l21 * z1
    y1 = over(z1, d1, h11)
    y0 = over(b0, h00, h00) - l10 * y1
    first = y0 * v[0] + y1 * v[1]
    second = v[2] - l21 * v[1] + (l10 * l21 - l20) * v[0]
    sum_along(1)
    h22 = jnp.sum(summed(1), axis=1, keepdims=True)
    out_ref[...] = first + over(z2, h22 - less, h22) * second

    for dx, dy in GROUPS:
        if (dx, dy) != (0, 0):
            halo_copy(dx, dy).wait_send()
    drain(recv_z_lo.at[0:6], send_z.at[0])
    drain(recv_z_hi.at[0:6], send_z.at[1])
    drain(marks.at[0:26], send_m)
    for a in range(ITERS):
        drain(recv_v.at[a, 0:26], send_v.at[a])
    for k in range(2):
        drain(recv_a.at[k, 0:mates], send_r.at[k])
        drain(recv_b.at[k, 0 : size_x - 1], send_r.at[2 + k])


def solution(mesh):
    sizes = tuple(mesh.shape[a] for a in AXES)
    plane = sizes[1] * sizes[2]

    def body(density, base_velocity, cells, offsets, target, stiffness, counts):
        vmem = pl.BlockSpec(memory_space=pltpu.VMEM)
        return pl.pallas_call(
            functools.partial(kernel, sizes),
            out_shape=jax.ShapeDtypeStruct((3, CAP), F32),
            in_specs=[pl.BlockSpec(memory_space=pl.ANY)] * 7,
            out_specs=vmem,
            scratch_shapes=[
                pltpu.SMEM((1,), jnp.int32),
                pltpu.VMEM((CX, CY, CZ), F32),
                pltpu.VMEM((3, CAP), jnp.int32),
                pltpu.VMEM((3, CAP), F32),
                pltpu.VMEM((3, CAP), F32),
                pltpu.VMEM((1, CAP), F32),
                pltpu.VMEM((CX, 4, CY, CZ), F32),
                pltpu.VMEM((CZ, 4 * CX * CY), F32),
                pltpu.VMEM((CX, 8, CZ), F32),
                pltpu.VMEM((CX, 16, CZ), F32),
                pltpu.VMEM((2, 4 * CX * CY), F32),
                pltpu.VMEM((4, 4 * CX * CY), F32),
                pltpu.VMEM((8, CAP), F32),
                pltpu.VMEM((2, CX, 4, CY, CZ), F32),
                pltpu.VMEM((3, CX, 8, CZ), F32),
                pltpu.VMEM((3, CX, 16, CZ), F32),
                pltpu.VMEM((9, 2, 4 * CX * CY), F32),
                pltpu.VMEM((9, 4, 4 * CX * CY), F32),
                pltpu.VMEM((8, 4 * CX * CY), F32),
                pltpu.VMEM((27, 8, CAP), F32),
                pltpu.VMEM((WX, 4, WY, CZ), F32),
                pltpu.VMEM((WX, 4, WY, CZ), F32),
                pltpu.VMEM((CX, 4, CY, CZ), F32),
                pltpu.VMEM((4, WX, WY, WZ), F32),
                pltpu.VMEM((9, TZ, CAP), BF16),
                pltpu.VMEM((9, TZ, CAP), BF16),
                pltpu.VMEM((WZ, CAP), BF16),
                pltpu.VMEM((WZ, CAP), BF16),
                pltpu.VMEM((sum(SPANS), CAP), F32),
                pltpu.VMEM((2, sum(SPANS), CAP), BF16),
                pltpu.VMEM((2, sum(SPANS), CAP), BF16),
                pltpu.VMEM((18, 16, CAP), F32),
                pltpu.VMEM((3 * max(SPANS), CAP), BF16),
                pltpu.VMEM((3 * max(SPANS), CAP), BF16),
                pltpu.VMEM((3, WX, WY, WZ), F32),
                pltpu.VMEM((WX, WY, CZ), F32),
                pltpu.VMEM((3, WX, WY, WZ), F32),
                pltpu.VMEM((3, WX, WY, WZ), F32),
                pltpu.VMEM((3, WX, WY, WZ), F32),
                pltpu.VMEM((2, WX, WY, WZ), F32),
                pltpu.VMEM((3, 11, WY, WZ), BF16),
                pltpu.VMEM((3, 11, WY, WZ), BF16),
                pltpu.VMEM((ITERS + 1, 4, CAP), F32),
                pltpu.VMEM((ITERS, 4, CAP), F32),
                pltpu.VMEM((ITERS, 27, 4, CAP), F32),
                pltpu.VMEM((2, 1, 128), F32),
                pltpu.VMEM((2, plane, 1, 128), F32),
                pltpu.VMEM((2, 1, 128), F32),
                pltpu.VMEM((2, sizes[0], 1, 128), F32),
                pltpu.SemaphoreType.DMA((9,)),
                pltpu.SemaphoreType.DMA((9,)),
                pltpu.SemaphoreType.DMA((9,)),
                pltpu.SemaphoreType.DMA((2,)),
                pltpu.SemaphoreType.DMA((2,)),
                pltpu.SemaphoreType.DMA,
                pltpu.SemaphoreType.DMA,
                pltpu.SemaphoreType.DMA((ITERS,)),
                pltpu.SemaphoreType.DMA((ITERS, 3)),
                pltpu.SemaphoreType.DMA((4,)),
                pltpu.SemaphoreType.DMA((4,)),
            ],
            compiler_params=pltpu.CompilerParams(
                collective_id=0, has_side_effects=True, vmem_limit_bytes=60 * 1024 * 1024
            ),
            name="immersed",
        )(density, base_velocity, cells, offsets, target, stiffness[None], counts)

    return jax.shard_map(
        body,
        mesh=mesh,
        in_specs=(
            P(*AXES), P(None, *AXES), P(None, ALL), P(None, ALL), P(None, ALL), P(ALL), P(ALL),
        ),
        out_specs=P(None, ALL),
        check_vma=False,
    )
```

```python
import functools

import jax
import jax.numpy as jnp
from jax import lax
from jax.experimental import pallas as pl
from jax.experimental.pallas import tpu as pltpu
from jax.sharding import PartitionSpec as P

ITERS = 3
CX, CY, CZ = 8, 8, 128
CAP = 256
WX, WY, WZ = 13, 16, 256
TZ = 144
AXES = ("gx", "gy", "gz")
ALL = ("gx", "gy", "gz")
MESH = pl.DeviceIdType.MESH
SHIFT = 0.1
F32, BF16 = jnp.float32, jnp.bfloat16

GROUPS = [(dx, dy) for dx in (-1, 0, 1) for dy in (-1, 0, 1)]
DZS = (-1, 1, 0)
ORDER = sorted(range(9), key=lambda g: abs(GROUPS[g][0]) + abs(GROUPS[g][1]))
PLANES = {-1: (0, 4), 0: (1, 12), 1: (9, 4)}
ROWS = {-1: (0, 8), 0: (0, 16), 1: (8, 8)}
TAKE = {-1: (6, 8), 0: (0, 8), 1: (0, 3)}
TAKE_BASE = {-1: (7, 8), 0: (0, 8), 1: (0, 2)}
MIDDLE = (5, 6, 7)
OUTER = (1, 2, 3, 4, 8, 9, 10, 11)
PLACE = {x: k for k, x in enumerate(OUTER + MIDDLE)}


def group_of(dx, dy):
    return (dx + 1) * 3 + dy + 1


def slot_of(dx, dy, dz):
    return group_of(dx, dy) * 3 + DZS.index(dz)


NEIGHBOURS = [
    (GROUPS[g][0], GROUPS[g][1], dz)
    for g in ORDER
    for dz in DZS
    if (GROUPS[g][0], GROUPS[g][1], dz) != (0, 0, 0)
]
NEIGHBOURS.sort(key=lambda offset: sum(map(abs, offset)))
CENTRE = group_of(0, 0)
SPANS = [PLANES[dx][1] * ROWS[dy][1] for dx, dy in GROUPS]
STARTS = [sum(SPANS[:g]) for g in range(9)]


def split(value):
    high = value.astype(BF16)
    return high, (value - high.astype(F32)).astype(BF16)


def dot3(lh, ll, rh, rl, dims):
    dot = functools.partial(
        lax.dot_general, dimension_numbers=(dims, ((), ())), preferred_element_type=F32
    )
    return dot(lh, rh) + (dot(ll, rh) + dot(lh, rl))


def kernel(
    sizes,
    density_in, base_in, cells_in, offsets_in, target_in, stiff_in, counts_in,
    out_ref,
    counts_ref,
    density_ref, cells_ref, offsets_ref, target_ref, stiff_ref,
    field, ftrans, pack_lo, pack_hi, spack_lo, spack_hi, pack_z_lo, pack_z_hi, mark_own,
    recv_x, recv_lo, recv_hi, srecv_x, srecv_lo, srecv_hi,
    recv_z_lo, recv_z_hi, columns, marks, main, halo, ztile, wide,
    table_h, table_l, own_h, own_l, wxy, wxy_h, wxy_l, edge_w, left_h, left_l, grid, edges, moved, plane_a, plane_b, plane_c,
    vel_h, vel_l, vecs, images, recv_v, part, recv_a, part_b, recv_b,
    loaded, send_f, got_f, send_s, got_s, send_z, got_z, send_m, got_m, send_v, got_v, send_r, got_r,
):
    size_x, size_y, size_z = sizes
    ix, iy, iz = (lax.axis_index(a) for a in AXES)

    def at(dx, dy, dz):
        return (
            lax.rem(ix + dx + size_x, size_x),
            lax.rem(iy + dy + size_y, size_y),
            lax.rem(iz + dz + size_z, size_z),
        )

    def mate(y, z):
        return (ix, lax.rem(iy + y, size_y), lax.rem(iz + z, size_z))

    def along(k):
        return (lax.rem(ix + k, size_x), iy, iz)

    loads = [
        pltpu.make_async_copy(base_in.at[c], field.at[:, c], loaded.at[c]) for c in range(3)
    ]
    loads += [
        pltpu.make_async_copy(source, target, loaded.at[3 + k])
        for k, (source, target) in enumerate(
            [
                (density_in, density_ref), (cells_in, cells_ref), (offsets_in, offsets_ref),
                (target_in, target_ref), (stiff_in, stiff_ref), (counts_in, counts_ref),
            ]
        )
    ]
    for load in loads:
        load.start()

    barrier = pltpu.get_barrier_semaphore()
    for offset in NEIGHBOURS:
        pl.semaphore_signal(barrier, inc=1, device_id=at(*offset), device_id_type=MESH)

    def greet_mate(k, carry):
        other = mate(k // size_z, lax.rem(k, size_z))
        pl.semaphore_signal(barrier, inc=1, device_id=other, device_id_type=MESH)
        return carry

    lax.fori_loop(1, size_y * size_z, greet_mate, 0)
    for k in range(1, size_x):
        pl.semaphore_signal(barrier, inc=1, device_id=along(k), device_id_type=MESH)

    for load in loads:
        load.wait()
    field[:, 3] = lax.rsqrt(density_ref[...])
    ftrans[...] = field[...].reshape(4 * CX * CY, CZ).T
    pack_z_lo[...] = ftrans[CZ - 2 : CZ]
    pack_z_hi[...] = ftrans[0:4]
    for c in range(3):
        pack_lo[:, c : c + 1] = field[:, c, CY - 1 : CY]
        pack_hi[:, 2 * c : 2 * c + 2] = field[:, c, 0:2]
    spack_lo[...] = field[:, 3, CY - 2 : CY]
    spack_hi[...] = field[:, 3, 0:4]
    anchors = (ix * CX, iy * CY, iz * CZ)
    for k in range(3):
        mark_own[k : k + 1] = (cells_ref[k : k + 1] - anchors[k]).astype(F32)
    mark_own[3:6] = offsets_ref[...]
    mark_own[6:8] = jnp.zeros((2, CAP), F32)
    marks[slot_of(0, 0, 0)] = mark_own[...]

    pl.semaphore_wait(barrier, len(NEIGHBOURS) + size_y * size_z - 1 + size_x - 1)

    def remote(src, dst, send, recv, device):
        return pltpu.make_async_remote_copy(
            src_ref=src, dst_ref=dst, send_sem=send, recv_sem=recv, device_id=device,
            device_id_type=MESH,
        )

    def drain(ref, sem):
        pltpu.make_async_copy(ref, ref, sem).wait()

    def halo_copy(dx, dy):
        a, b = TAKE_BASE[-dx]
        g = group_of(-dx, -dy)
        if dy == 0:
            pair = field.at[a:b, 0:3], recv_x.at[(1 - dx) // 2, a:b]
        elif dy == 1:
            pair = pack_lo.at[a:b], recv_lo.at[1 - dx, a:b]
        else:
            pair = pack_hi.at[a:b], recv_hi.at[1 - dx, a:b]
        return remote(*pair, send_f.at[g], got_f.at[g], at(dx, dy, 0))

    def scale_copy(dx, dy):
        a, b = TAKE[-dx]
        g = group_of(-dx, -dy)
        if dy == 0:
            pair = field.at[a:b, 3], srecv_x.at[(1 - dx) // 2, a:b]
        elif dy == 1:
            pair = spack_lo.at[a:b], srecv_lo.at[1 - dx, a:b]
        else:
            pair = spack_hi.at[a:b], srecv_hi.at[1 - dx, a:b]
        return remote(*pair, send_s.at[g], got_s.at[g], at(dx, dy, 0))

    def edge_copy(dx, dy, dz):
        a, b = {-1: (0, 128), 0: (0, 256), 1: (128, 256)}[dx]
        g = group_of(-dx, -dy)
        if dz == 1:
            pair = pack_z_lo.at[:, a:b], recv_z_lo.at[g, :, a:b]
        else:
            pair = pack_z_hi.at[:, a:b], recv_z_hi.at[g, :, a:b]
        side = (1 - dz) // 2
        return remote(*pair, send_z.at[side], got_z.at[side], at(dx, dy, dz))

    around = [GROUPS[g] for g in reversed(ORDER) if g != CENTRE]
    for dx, dy, dz in NEIGHBOURS:
        if dz:
            edge_copy(dx, dy, dz).start()
    for dx, dy in around:
        halo_copy(dx, dy).start()
    for dx, dy in around:
        scale_copy(dx, dy).start()
    for dx, dy, dz in NEIGHBOURS:
        back = slot_of(-dx, -dy, -dz)
        remote(mark_own, marks.at[back], send_m, got_m, at(dx, dy, dz)).start()

    own_h[...] = jnp.zeros(own_h.shape, BF16)
    own_l[...] = jnp.zeros(own_l.shape, BF16)
    ztile[...] = jnp.zeros(ztile.shape, F32)
    columns[...] = jnp.zeros(columns.shape, F32)
    main[...] = jnp.zeros(main.shape, F32)
    halo[:, :, 8:16] = jnp.zeros((WX, 4, 8, CZ), F32)
    grid[...] = jnp.zeros(grid.shape, F32)
    edges[...] = jnp.zeros(edges.shape, F32)
    vecs[...] = jnp.zeros(vecs.shape, F32)

    live = (lax.broadcasted_iota(jnp.int32, (1, CAP), 1) < counts_ref[0]).astype(F32)
    stiff = stiff_ref[...]

    def axis_table(first, rows, start, weights):
        away = (
            lax.broadcasted_iota(jnp.int32, (rows, CAP), 0).astype(F32) + float(first) - start
        )
        value = jnp.zeros((rows, CAP), F32)
        for step in range(4):
            value = jnp.where(away == float(step), weights[step], value)
        return value

    def build(g, j):
        (dx, dy), dz = GROUPS[g], DZS[j]
        mark = marks[g * 3 + j]
        fraction = mark[3:6]
        root = jnp.sqrt(1.0 + 4.0 * fraction - 4.0 * fraction * fraction)
        weights = [
            (3.0 - 2.0 * fraction - root) * 0.125,
            (3.0 - 2.0 * fraction + root) * 0.125,
            (1.0 + 2.0 * fraction + root) * 0.125,
            (1.0 + 2.0 * fraction - root) * 0.125,
        ]
        of = lambda k: [w[k : k + 1] for w in weights]
        x0, nx = PLANES[dx]
        y0, ny = ROWS[dy]
        table_x = axis_table(x0, 16, mark[0:1] + float(1 + CX * dx), of(0))
        table_y = axis_table(y0, ny, mark[1:2] + float(1 + CY * dy), of(1))
        for x in range(nx):
            rows = slice(STARTS[g] + x * ny, STARTS[g] + (x + 1) * ny)
            weight = table_x[x : x + 1] * table_y
            if dz == 0:
                wxy[rows] = weight
            else:
                high, low = split(weight)
                wxy_h[j, rows] = high
                wxy_l[j, rows] = low
        start = mark[2:3] + float(1 + CZ * dz)
        if dz == 0:
            high, low = split(axis_table(0, TZ, start, of(2)))
            table_h[g] = high
            table_l[g] = low
            if g == CENTRE:
                own_h[0:TZ] = high
                own_l[0:TZ] = low
        else:
            touched = axis_table({-1: 0, 1: CZ + 1}[dz], 8, start, of(2))[0:4]
            edge_w[2 * g + j, 0:12] = jnp.concatenate([touched] * 3, axis=0)
            edge_w[2 * g + j, 12:16] = jnp.zeros((4, CAP), F32)

    build(CENTRE, 2)

    lane = lax.broadcasted_iota(jnp.int32, (WY, CZ), 1)

    def place(takes, comps, centre, sides, low, high, low_step, high_step):
        for g, (dx, dy) in enumerate(GROUPS):
            (xa, xb), (ya, yb) = takes[dx], takes[dy]
            x0, y0 = xa + CX * dx + 2, ya + CY * dy + 2
            planes, rows = slice(x0, x0 + xb - xa), slice(y0, y0 + yb - ya)
            for k, c in enumerate(comps):
                if g == CENTRE:
                    main[planes, c, rows] = centre[:, c]
                elif dy == 0:
                    main[planes, c, rows] = sides(dx, slice(xa, xb), k)
                elif dy == -1:
                    first = k * low_step
                    main[planes, c, rows] = low[dx + 1, xa:xb, first : first + yb - ya]
                else:
                    first = k * high_step
                    main[planes, c, rows] = high[dx + 1, xa:xb, first : first + yb - ya]

    def widened(x, c):
        turned = pltpu.roll(main[x, c], 2, 1)
        edge = halo[x, c]
        head = jnp.where(lane < 2, edge, turned)
        tail = jnp.where(lane < 2, turned, jnp.where(lane < 5, edge, 0.0))
        return jnp.concatenate([head, tail], axis=1)

    for dx, dy in around:
        halo_copy(dx, dy).wait_recv()
    place(
        TAKE_BASE, (0, 1, 2), field, lambda dx, planes, k: recv_x[(dx + 1) // 2, planes, k],
        recv_lo, recv_hi, 1, 2,
    )
    drain(recv_z_lo.at[0:6], got_z.at[0])
    drain(recv_z_hi.at[0:6], got_z.at[1])
    for g, (dx, dy) in enumerate(GROUPS):
        (xa, xb), (ya, yb) = TAKE[dx], TAKE[dy]
        x0, y0 = xa + CX * dx + 2, ya + CY * dy + 2
        columns[0:2] = recv_z_lo[g]
        columns[2:6] = recv_z_hi[g]
        ztile[:, :, :, 0:8] = columns[...].T.reshape(CX, 4, CY, 8)
        halo[x0 : x0 + xb - xa, :, y0 : y0 + yb - ya] = ztile[xa:xb, :, ya:yb]

    def interpolate(planes):
        first, count = PLACE[planes[0]], len(planes)
        span = count * WY
        rows = dot3(
            vel_h[:, first : first + count].reshape(3 * span, WZ),
            vel_l[:, first : first + count].reshape(3 * span, WZ),
            own_h[...], own_l[...], ((1,), (0,)),
        )
        starts = [STARTS[CENTRE] + (x - 1) * WY for x in planes]
        weight = jnp.concatenate([wxy[start : start + WY] for start in starts], axis=0)
        return [
            jnp.sum(rows[c * span : (c + 1) * span] * weight, axis=0, keepdims=True)
            for c in range(3)
        ]

    for x in range(1, 12):
        for c in range(3):
            high, low = split(widened(x, c))
            vel_h[c, PLACE[x]] = high
            vel_l[c, PLACE[x]] = low
    for c, value in enumerate(interpolate(OUTER + MIDDLE)):
        vecs[0, c : c + 1] = live * (target_ref[c : c + 1] - value)

    def send_vector(a):
        for dx, dy, dz in NEIGHBOURS:
            back = slot_of(-dx, -dy, -dz)
            remote(
                vecs.at[a], recv_v.at[a, back], send_v.at[a], got_v.at[a, abs(dx) + abs(dy) + abs(dz) - 1],
                at(dx, dy, dz),
            ).start()
        recv_v[a, slot_of(0, 0, 0)] = vecs[a]

    part_row = lax.broadcasted_iota(jnp.int32, (16, CAP), 0)

    def spread_inner(a, g):
        span = SPANS[g]
        vector = recv_v[a, 3 * g + 2]
        weight = wxy[STARTS[g] : STARTS[g] + span]
        for c in range(3):
            high, low = split(weight * vector[c : c + 1])
            left_h[c * span : (c + 1) * span] = high
            left_l[c * span : (c + 1) * span] = low
        return dot3(left_h[0 : 3 * span], left_l[0 : 3 * span], table_h[g], table_l[g], ((1,), (1,)))

    def spread_edges(a, g):
        rows = slice(STARTS[g], STARTS[g] + SPANS[g])
        sides = []
        for j in range(2):
            vector = recv_v[a, 3 * g + j]
            value = jnp.where(
                part_row < 4, vector[0:1], jnp.where(part_row < 8, vector[1:2], vector[2:3])
            )
            high, low = split(edge_w[2 * g + j] * value)
            sides.append(dot3(high, low, wxy_h[j, rows], wxy_l[j, rows], ((1,), (1,))))
        return jnp.concatenate(sides, axis=0).T

    def add_inner(a, g):
        (dx, dy), span = GROUPS[g], SPANS[g]
        x0, nx = PLANES[dx]
        y0, ny = ROWS[dy]
        total = spread_inner(a, g)
        for c in range(3):
            at_place = (c, slice(x0, x0 + nx), slice(y0, y0 + ny), slice(0, TZ))
            grid[at_place] += total[c * span : (c + 1) * span].reshape(nx, ny, TZ)

    def add_edges(a, g):
        dx, dy = GROUPS[g]
        x0, nx = PLANES[dx]
        y0, ny = ROWS[dy]
        edges[x0 : x0 + nx, y0 : y0 + ny, 0:32] += spread_edges(a, g).reshape(nx, ny, 32)

    def spread(a, middle):
        far = [abs(dx) + abs(dy) for dx, dy in GROUPS]
        grid[:, :, :, 0:TZ] = jnp.zeros((3, WX, WY, TZ), F32)
        edges[:, :, 0:32] = jnp.zeros((WX, WY, 32), F32)
        kept = None
        for hops, messages in enumerate((0, 6, 12, 8)):
            if hops:
                drain(recv_v.at[a, 0:messages], got_v.at[a, hops - 1])
            if hops == 3:
                kept = middle()
            for g in range(9):
                if far[g] == hops:
                    add_inner(a, g)
            for g in range(9):
                if far[g] == hops - 1:
                    add_edges(a, g)
        return kept

    def shifts(value, axis):
        length = value.shape[axis]
        return pltpu.roll(value, 1, axis), pltpu.roll(value, length - 1, axis)

    def both(value, axis):
        before, after = shifts(value, axis)
        return before + after

    def stream(last, planes, outputs, energy):
        for x in planes:
            scale = wide[x]
            edge = edges[x]
            values = []
            for c in range(3):
                head = grid[c, x, :, 0:CZ] + jnp.where(
                    lane < 4, pltpu.roll(edge, CZ - 4 * c, 1) if c else edge, 0.0
                )
                tail = grid[c, x, :, CZ:] + jnp.where(
                    (lane > 0) & (lane < 5), pltpu.roll(edge, CZ - 15 - 4 * c, 1), 0.0
                )
                values.append(scale * jnp.concatenate([head, tail], axis=1))
            m0, m1, m2 = values
            moved[0, x], moved[1, x], moved[2, x] = m0, m1, m2
            before, after = shifts(m0, 0)
            sy0, dy0 = before + after, before - after
            before, after = shifts(m1, 0)
            sy1, dy1 = before + after, before - after
            before, after = shifts(m0, 1)
            sz0, dz0 = before + after, before - after
            before, after = shifts(m2, 1)
            sz2, dz2 = before + after, before - after
            before, after = shifts(dz2, 0)
            dyz2 = before - after
            before, after = shifts(dy1, 1)
            dyz1 = before - after
            plane_a[0, x] = 2.0 * m0 + sy0 + sz0
            plane_b[0, x] = dy1 + dz2
            plane_a[1, x] = sy1
            plane_b[1, x] = dy0
            plane_c[0, x] = 2.0 * sy1 + both(sy1, 1) + dyz2
            plane_a[2, x] = sz2
            plane_b[2, x] = dz0
            plane_c[1, x] = 2.0 * sz2 + both(sz2, 0) + dyz1

        for x in outputs:
            half = wide[x] * 0.5
            for c in range(3):
                post = plane_a[c, x - 1] + plane_a[c, x + 1] + plane_b[c, x - 1] - plane_b[c, x + 1]
                if c:
                    post = post + plane_c[c - 1, x]
                response = moved[c, x] + post * (1.0 / 12.0)
                if last:
                    energy = energy + moved[c, x] * response
                else:
                    high, low = split(half * response)
                    vel_h[c, PLACE[x]] = high
                    vel_l[c, PLACE[x]] = low
        return energy

    lane_row = lax.broadcasted_iota(jnp.int32, (1, 128), 1)
    me = iy * size_z + iz
    mates = size_y * size_z - 1
    far_mates = [(y, z) for y in range(size_y) for z in range(size_z) if (y, z) != (0, 0)]
    far_mates.sort(key=lambda k: -(min(k[0], size_y - k[0]) / 2 + min(k[1], size_z - k[1])))

    def sum_plane(k, row):
        part[k] = row
        recv_a[k, me] = row
        for other in far_mates:
            remote(part.at[k], recv_a.at[k, me], send_r.at[k], got_r.at[k], mate(*other)).start()

    def sum_along(k):
        drain(recv_a.at[k, 0:mates], got_r.at[k])
        row = jnp.sum(recv_a[k], axis=0)
        part_b[k] = row
        recv_b[k, ix] = row
        for other in sorted(range(1, size_x), key=lambda k: -min(k, size_x - k)):
            remote(
                part_b.at[k], recv_b.at[k, ix], send_r.at[2 + k], got_r.at[2 + k], along(other)
            ).start()

    def summed(k):
        drain(recv_b.at[k, 0 : size_x - 1], got_r.at[2 + k])
        return jnp.sum(recv_b[k], axis=0)

    for a in range(ITERS):
        send_vector(a)
        if a == 0:
            for dx, dy in around:
                scale_copy(dx, dy).wait_recv()
            place(
                TAKE, (3,), field, lambda dx, planes, k: srecv_x[(dx + 1) // 2, planes],
                srecv_lo, srecv_hi, 0, 0,
            )
            for x in range(WX):
                wide[x] = widened(x, 3)
            drain(marks.at[0:26], got_m)
            for g in ORDER:
                for j in range(3):
                    if (g, j) != (CENTRE, 2):
                        build(g, j)
        last = a == ITERS - 1
        if last:
            v = [vecs[k, 0:3] for k in range(3)]
            w = [images[k, 0:3] for k in range(2)]
            pairs = [(v[0], w[0]), (v[0], w[1]), (v[2], w[0]), (v[1], w[1]), (v[2], w[1])]
            pairs = pairs + [(v[0], v[j]) for j in range(3)]
            row = jnp.zeros((1, 128), F32)
            for k, (left, right) in enumerate(pairs):
                row = jnp.where(lane_row == k, jnp.sum(left * right), row)
            sum_plane(0, row)

        def middle():
            energy = stream(last, range(4, 9), MIDDLE, jnp.zeros((WY, WZ), F32))
            return energy if last else interpolate(MIDDLE)

        kept = spread(a, middle)
        if last:
            sum_along(0)
            energy = stream(last, (1, 2, 3, 9, 10), (2, 3, 4, 8, 9), kept)
        else:
            stream(last, (0, 1, 2, 3, 9, 10, 11, 12), OUTER, None)
            for c, value in enumerate(interpolate(OUTER)):
                vector = vecs[a, c : c + 1]
                image = live * (kept[c] + value + stiff * vector)
                images[a, c : c + 1] = image
                vecs[a + 1, c : c + 1] = image - SHIFT * vector

    inside = lambda axis, size: (
        lax.broadcasted_iota(jnp.int32, (WY, WZ), axis) - 2
    ).astype(jnp.uint32) < size
    energy = jnp.where(inside(0, CY) & inside(1, CZ), energy, 0.0)
    own = jnp.sum(0.5 * energy, axis=0, keepdims=True)
    own = own + jnp.sum(stiff * v[2] * v[2], axis=0, keepdims=True)
    sum_plane(1, own[:, 0:128] + own[:, 128:256])
    total = summed(0)
    h00, h01, h02, h11, h12, b0, b1, b2 = (
        jnp.sum(jnp.where(lane_row == k, total, 0.0), axis=1, keepdims=True) for k in range(8)
    )

    def over(top, pivot, size):
        fine = pivot > 1e-7 * size
        return jnp.where(fine, top / jnp.where(fine, pivot, 1.0), 0.0)

    l10 = over(h01, h00, h00)
    l20 = over(h02, h00, h00)
    d1 = h11 - l10 * h01
    e12 = h12 - l10 * h02
    l21 = over(e12, d1, h11)
    less = h02 * l20 + l21 * e12
    z1 = b1 - l10 * b0
    z2 = b2 - l20 * b0 - l21 * z1
    y1 = over(z1, d1, h11)
    y0 = over(b0, h00, h00) - l10 * y1
    first = y0 * v[0] + y1 * v[1]
    second = v[2] - l21 * v[1] + (l10 * l21 - l20) * v[0]
    sum_along(1)
    h22 = jnp.sum(summed(1), axis=1, keepdims=True)
    out_ref[...] = first + over(z2, h22 - less, h22) * second

    for dx, dy in GROUPS:
        if (dx, dy) != (0, 0):
            halo_copy(dx, dy).wait_send()
            scale_copy(dx, dy).wait_send()
    drain(recv_z_lo.at[0:6], send_z.at[0])
    drain(recv_z_hi.at[0:6], send_z.at[1])
    drain(marks.at[0:26], send_m)
    for a in range(ITERS):
        drain(recv_v.at[a, 0:26], send_v.at[a])
    for k in range(2):
        drain(recv_a.at[k, 0:mates], send_r.at[k])
        drain(recv_b.at[k, 0 : size_x - 1], send_r.at[2 + k])


def solution(mesh):
    sizes = tuple(mesh.shape[a] for a in AXES)
    plane = sizes[1] * sizes[2]

    def body(density, base_velocity, cells, offsets, target, stiffness, counts):
        vmem = pl.BlockSpec(memory_space=pltpu.VMEM)
        return pl.pallas_call(
            functools.partial(kernel, sizes),
            out_shape=jax.ShapeDtypeStruct((3, CAP), F32),
            in_specs=[pl.BlockSpec(memory_space=pl.ANY)] * 7,
            out_specs=vmem,
            scratch_shapes=[
                pltpu.SMEM((1,), jnp.int32),
                pltpu.VMEM((CX, CY, CZ), F32),
                pltpu.VMEM((3, CAP), jnp.int32),
                pltpu.VMEM((3, CAP), F32),
                pltpu.VMEM((3, CAP), F32),
                pltpu.VMEM((1, CAP), F32),
                pltpu.VMEM((CX, 4, CY, CZ), F32),
                pltpu.VMEM((CZ, 4 * CX * CY), F32),
                pltpu.VMEM((CX, 4, CZ), F32),
                pltpu.VMEM((CX, 8, CZ), F32),
                pltpu.VMEM((CX, 2, CZ), F32),
                pltpu.VMEM((CX, 4, CZ), F32),
                pltpu.VMEM((2, 4 * CX * CY), F32),
                pltpu.VMEM((4, 4 * CX * CY), F32),
                pltpu.VMEM((8, CAP), F32),
                pltpu.VMEM((2, CX, 3, CY, CZ), F32),
                pltpu.VMEM((3, CX, 4, CZ), F32),
                pltpu.VMEM((3, CX, 8, CZ), F32),
                pltpu.VMEM((2, CX, CY, CZ), F32),
                pltpu.VMEM((3, CX, 2, CZ), F32),
                pltpu.VMEM((3, CX, 4, CZ), F32),
                pltpu.VMEM((9, 2, 4 * CX * CY), F32),
                pltpu.VMEM((9, 4, 4 * CX * CY), F32),
                pltpu.VMEM((8, 4 * CX * CY), F32),
                pltpu.VMEM((27, 8, CAP), F32),
                pltpu.VMEM((WX, 4, WY, CZ), F32),
                pltpu.VMEM((WX, 4, WY, CZ), F32),
                pltpu.VMEM((CX, 4, CY, CZ), F32),
                pltpu.VMEM((WX, WY, WZ), F32),
                pltpu.VMEM((9, TZ, CAP), BF16),
                pltpu.VMEM((9, TZ, CAP), BF16),
                pltpu.VMEM((WZ, CAP), BF16),
                pltpu.VMEM((WZ, CAP), BF16),
                pltpu.VMEM((sum(SPANS), CAP), F32),
                pltpu.VMEM((2, sum(SPANS), CAP), BF16),
                pltpu.VMEM((2, sum(SPANS), CAP), BF16),
                pltpu.VMEM((18, 16, CAP), F32),
                pltpu.VMEM((3 * max(SPANS), CAP), BF16),
                pltpu.VMEM((3 * max(SPANS), CAP), BF16),
                pltpu.VMEM((3, WX, WY, WZ), F32),
                pltpu.VMEM((WX, WY, CZ), F32),
                pltpu.VMEM((3, WX, WY, WZ), F32),
                pltpu.VMEM((3, WX, WY, WZ), F32),
                pltpu.VMEM((3, WX, WY, WZ), F32),
                pltpu.VMEM((2, WX, WY, WZ), F32),
                pltpu.VMEM((3, 11, WY, WZ), BF16),
                pltpu.VMEM((3, 11, WY, WZ), BF16),
                pltpu.VMEM((ITERS + 1, 4, CAP), F32),
                pltpu.VMEM((ITERS, 4, CAP), F32),
                pltpu.VMEM((ITERS, 27, 4, CAP), F32),
                pltpu.VMEM((2, 1, 128), F32),
                pltpu.VMEM((2, plane, 1, 128), F32),
                pltpu.VMEM((2, 1, 128), F32),
                pltpu.VMEM((2, sizes[0], 1, 128), F32),
                pltpu.SemaphoreType.DMA((9,)),
                pltpu.SemaphoreType.DMA((9,)),
                pltpu.SemaphoreType.DMA((9,)),
                pltpu.SemaphoreType.DMA((9,)),
                pltpu.SemaphoreType.DMA((9,)),
                pltpu.SemaphoreType.DMA((2,)),
                pltpu.SemaphoreType.DMA((2,)),
                pltpu.SemaphoreType.DMA,
                pltpu.SemaphoreType.DMA,
                pltpu.SemaphoreType.DMA((ITERS,)),
                pltpu.SemaphoreType.DMA((ITERS, 3)),
                pltpu.SemaphoreType.DMA((4,)),
                pltpu.SemaphoreType.DMA((4,)),
            ],
            compiler_params=pltpu.CompilerParams(
                collective_id=0, has_side_effects=True, vmem_limit_bytes=60 * 1024 * 1024
            ),
            name="immersed",
        )(density, base_velocity, cells, offsets, target, stiffness[None], counts)

    return jax.shard_map(
        body,
        mesh=mesh,
        in_specs=(
            P(*AXES), P(None, *AXES), P(None, ALL), P(None, ALL), P(None, ALL), P(ALL), P(ALL),
        ),
        out_specs=P(None, ALL),
        check_vma=False,
    )
```

```python
import functools

import jax
import jax.numpy as jnp
from jax import lax
from jax.experimental import pallas as pl
from jax.experimental.pallas import tpu as pltpu
from jax.sharding import PartitionSpec as P

ITERS = 3
CX, CY, CZ = 8, 8, 128
CAP = 256
WX, WY, WZ = 13, 16, 256
TZ = 144
AXES = ("gx", "gy", "gz")
ALL = ("gx", "gy", "gz")
MESH = pl.DeviceIdType.MESH
SHIFT = 0.1
F32, BF16 = jnp.float32, jnp.bfloat16

GROUPS = [(dx, dy) for dx in (-1, 0, 1) for dy in (-1, 0, 1)]
DZS = (-1, 1, 0)
ORDER = sorted(range(9), key=lambda g: abs(GROUPS[g][0]) + abs(GROUPS[g][1]))
PLANES = {-1: (0, 4), 0: (1, 12), 1: (9, 4)}
ROWS = {-1: (0, 8), 0: (0, 16), 1: (8, 8)}
TAKE = {-1: (6, 8), 0: (0, 8), 1: (0, 3)}
TAKE_BASE = {-1: (7, 8), 0: (0, 8), 1: (0, 2)}
MIDDLE = (5, 6, 7)
OUTER = (1, 2, 3, 4, 8, 9, 10, 11)
PLACE = {x: k for k, x in enumerate(OUTER + MIDDLE)}


def group_of(dx, dy):
    return (dx + 1) * 3 + dy + 1


def slot_of(dx, dy, dz):
    return group_of(dx, dy) * 3 + DZS.index(dz)


NEIGHBOURS = [
    (GROUPS[g][0], GROUPS[g][1], dz)
    for g in ORDER
    for dz in DZS
    if (GROUPS[g][0], GROUPS[g][1], dz) != (0, 0, 0)
]
NEIGHBOURS.sort(key=lambda offset: sum(map(abs, offset)))
CENTRE = group_of(0, 0)
SPANS = [PLANES[dx][1] * ROWS[dy][1] for dx, dy in GROUPS]
STARTS = [sum(SPANS[:g]) for g in range(9)]


def split(value):
    high = value.astype(BF16)
    return high, (value - high.astype(F32)).astype(BF16)


def dot3(lh, ll, rh, rl, dims):
    dot = functools.partial(
        lax.dot_general, dimension_numbers=(dims, ((), ())), preferred_element_type=F32
    )
    count = lh.shape[0]
    both = dot(jnp.concatenate([lh, ll], axis=0), rh)
    return both[:count] + (both[count:] + dot(lh, rl))


def kernel(
    sizes,
    density_in, base_in, cells_in, offsets_in, target_in, stiff_in, counts_in,
    out_ref,
    counts_ref,
    density_ref, cells_ref, offsets_ref, target_ref, stiff_ref,
    field, ftrans, pack_lo, pack_hi, spack_lo, spack_hi, pack_z_lo, pack_z_hi, mark_own,
    recv_x, recv_lo, recv_hi, srecv_x, srecv_lo, srecv_hi,
    recv_z_lo, recv_z_hi, columns, marks, main, halo, ztile, wide,
    table_h, table_l, own_h, own_l, wxy, wxy_h, wxy_l, edge_w, left_h, left_l, grid, edges, moved, plane_a, plane_b, plane_c,
    vel_h, vel_l, vecs, images, recv_v, part, recv_a, part_b, recv_b,
    loaded, send_f, got_f, send_s, got_s, send_z, got_z, send_m, got_m, send_v, got_v, send_r, got_r,
):
    size_x, size_y, size_z = sizes
    ix, iy, iz = (lax.axis_index(a) for a in AXES)

    def at(dx, dy, dz):
        return (
            lax.rem(ix + dx + size_x, size_x),
            lax.rem(iy + dy + size_y, size_y),
            lax.rem(iz + dz + size_z, size_z),
        )

    def mate(y, z):
        return (ix, lax.rem(iy + y, size_y), lax.rem(iz + z, size_z))

    def along(k):
        return (lax.rem(ix + k, size_x), iy, iz)

    loads = [
        pltpu.make_async_copy(base_in.at[c], field.at[:, c], loaded.at[c]) for c in range(3)
    ]
    loads += [
        pltpu.make_async_copy(source, target, loaded.at[3 + k])
        for k, (source, target) in enumerate(
            [
                (density_in, density_ref), (cells_in, cells_ref), (offsets_in, offsets_ref),
                (target_in, target_ref), (stiff_in, stiff_ref), (counts_in, counts_ref),
            ]
        )
    ]
    for load in loads:
        load.start()

    barrier = pltpu.get_barrier_semaphore()
    for offset in NEIGHBOURS:
        pl.semaphore_signal(barrier, inc=1, device_id=at(*offset), device_id_type=MESH)

    for load in loads:
        load.wait()
    field[:, 3] = lax.rsqrt(density_ref[...])
    ftrans[...] = field[...].reshape(4 * CX * CY, CZ).T
    pack_z_lo[...] = ftrans[CZ - 2 : CZ]
    pack_z_hi[...] = ftrans[0:4]
    for c in range(3):
        pack_lo[:, c : c + 1] = field[:, c, CY - 1 : CY]
        pack_hi[:, 2 * c : 2 * c + 2] = field[:, c, 0:2]
    spack_lo[...] = field[:, 3, CY - 2 : CY]
    spack_hi[...] = field[:, 3, 0:4]
    anchors = (ix * CX, iy * CY, iz * CZ)
    for k in range(3):
        mark_own[k : k + 1] = (cells_ref[k : k + 1] - anchors[k]).astype(F32)
    mark_own[3:6] = offsets_ref[...]
    mark_own[6:8] = jnp.zeros((2, CAP), F32)
    marks[slot_of(0, 0, 0)] = mark_own[...]

    pl.semaphore_wait(barrier, len(NEIGHBOURS))

    def remote(src, dst, send, recv, device):
        return pltpu.make_async_remote_copy(
            src_ref=src, dst_ref=dst, send_sem=send, recv_sem=recv, device_id=device,
            device_id_type=MESH,
        )

    def drain(ref, sem):
        pltpu.make_async_copy(ref, ref, sem).wait()

    def halo_copy(dx, dy):
        a, b = TAKE_BASE[-dx]
        g = group_of(-dx, -dy)
        if dy == 0:
            pair = field.at[a:b, 0:3], recv_x.at[(1 - dx) // 2, a:b]
        elif dy == 1:
            pair = pack_lo.at[a:b], recv_lo.at[1 - dx, a:b]
        else:
            pair = pack_hi.at[a:b], recv_hi.at[1 - dx, a:b]
        return remote(*pair, send_f.at[g], got_f.at[g], at(dx, dy, 0))

    def scale_copy(dx, dy):
        a, b = TAKE[-dx]
        g = group_of(-dx, -dy)
        if dy == 0:
            pair = field.at[a:b, 3], srecv_x.at[(1 - dx) // 2, a:b]
        elif dy == 1:
            pair = spack_lo.at[a:b], srecv_lo.at[1 - dx, a:b]
        else:
            pair = spack_hi.at[a:b], srecv_hi.at[1 - dx, a:b]
        return remote(*pair, send_s.at[g], got_s.at[g], at(dx, dy, 0))

    def edge_copy(dx, dy, dz):
        a, b = {-1: (0, 128), 0: (0, 256), 1: (128, 256)}[dx]
        g = group_of(-dx, -dy)
        if dz == 1:
            pair = pack_z_lo.at[:, a:b], recv_z_lo.at[g, :, a:b]
        else:
            pair = pack_z_hi.at[:, a:b], recv_z_hi.at[g, :, a:b]
        side = (1 - dz) // 2
        return remote(*pair, send_z.at[side], got_z.at[side], at(dx, dy, dz))

    around = [GROUPS[g] for g in reversed(ORDER) if g != CENTRE]
    for dx, dy, dz in NEIGHBOURS:
        if dz:
            edge_copy(dx, dy, dz).start()
    for dx, dy in around:
        halo_copy(dx, dy).start()
    for dx, dy in around:
        scale_copy(dx, dy).start()
    for dx, dy, dz in NEIGHBOURS:
        back = slot_of(-dx, -dy, -dz)
        remote(mark_own, marks.at[back], send_m, got_m, at(dx, dy, dz)).start()

    own_h[...] = jnp.zeros(own_h.shape, BF16)
    own_l[...] = jnp.zeros(own_l.shape, BF16)
    ztile[...] = jnp.zeros(ztile.shape, F32)
    columns[...] = jnp.zeros(columns.shape, F32)
    main[...] = jnp.zeros(main.shape, F32)
    halo[:, :, 8:16] = jnp.zeros((WX, 4, 8, CZ), F32)
    grid[...] = jnp.zeros(grid.shape, F32)
    edges[...] = jnp.zeros(edges.shape, F32)
    vecs[...] = jnp.zeros(vecs.shape, F32)

    live = (lax.broadcasted_iota(jnp.int32, (1, CAP), 1) < counts_ref[0]).astype(F32)
    stiff = stiff_ref[...]

    def axis_table(first, rows, start, weights):
        away = (
            lax.broadcasted_iota(jnp.int32, (rows, CAP), 0).astype(F32) + float(first) - start
        )
        value = jnp.zeros((rows, CAP), F32)
        for step in range(4):
            value = jnp.where(away == float(step), weights[step], value)
        return value

    def build(g, j):
        (dx, dy), dz = GROUPS[g], DZS[j]
        mark = marks[g * 3 + j]
        fraction = mark[3:6]
        root = jnp.sqrt(1.0 + 4.0 * fraction - 4.0 * fraction * fraction)
        weights = [
            (3.0 - 2.0 * fraction - root) * 0.125,
            (3.0 - 2.0 * fraction + root) * 0.125,
            (1.0 + 2.0 * fraction + root) * 0.125,
            (1.0 + 2.0 * fraction - root) * 0.125,
        ]
        of = lambda k: [w[k : k + 1] for w in weights]
        x0, nx = PLANES[dx]
        y0, ny = ROWS[dy]
        table_x = axis_table(x0, 16, mark[0:1] + float(1 + CX * dx), of(0))
        table_y = axis_table(y0, ny, mark[1:2] + float(1 + CY * dy), of(1))
        for x in range(nx):
            rows = slice(STARTS[g] + x * ny, STARTS[g] + (x + 1) * ny)
            weight = table_x[x : x + 1] * table_y
            if dz == 0:
                wxy[rows] = weight
            else:
                high, low = split(weight)
                wxy_h[j, rows] = high
                wxy_l[j, rows] = low
        start = mark[2:3] + float(1 + CZ * dz)
        if dz == 0:
            high, low = split(axis_table(0, TZ, start, of(2)))
            table_h[g] = high
            table_l[g] = low
            if g == CENTRE:
                own_h[0:TZ] = high
                own_l[0:TZ] = low
        else:
            touched = axis_table({-1: 0, 1: CZ + 1}[dz], 8, start, of(2))[0:4]
            edge_w[2 * g + j, 0:12] = jnp.concatenate([touched] * 3, axis=0)
            edge_w[2 * g + j, 12:16] = jnp.zeros((4, CAP), F32)

    build(CENTRE, 2)

    lane = lax.broadcasted_iota(jnp.int32, (WY, CZ), 1)

    def place(takes, comps, centre, sides, low, high, low_step, high_step):
        for g, (dx, dy) in enumerate(GROUPS):
            (xa, xb), (ya, yb) = takes[dx], takes[dy]
            x0, y0 = xa + CX * dx + 2, ya + CY * dy + 2
            planes, rows = slice(x0, x0 + xb - xa), slice(y0, y0 + yb - ya)
            for k, c in enumerate(comps):
                if g == CENTRE:
                    main[planes, c, rows] = centre[:, c]
                elif dy == 0:
                    main[planes, c, rows] = sides(dx, slice(xa, xb), k)
                elif dy == -1:
                    first = k * low_step
                    main[planes, c, rows] = low[dx + 1, xa:xb, first : first + yb - ya]
                else:
                    first = k * high_step
                    main[planes, c, rows] = high[dx + 1, xa:xb, first : first + yb - ya]

    def widened(x, c):
        turned = pltpu.roll(main[x, c], 2, 1)
        edge = halo[x, c]
        head = jnp.where(lane < 2, edge, turned)
        tail = jnp.where(lane < 2, turned, jnp.where(lane < 5, edge, 0.0))
        return jnp.concatenate([head, tail], axis=1)

    for dx, dy in around:
        halo_copy(dx, dy).wait_recv()
    place(
        TAKE_BASE, (0, 1, 2), field, lambda dx, planes, k: recv_x[(dx + 1) // 2, planes, k],
        recv_lo, recv_hi, 1, 2,
    )
    drain(recv_z_lo.at[0:6], got_z.at[0])
    drain(recv_z_hi.at[0:6], got_z.at[1])
    for g, (dx, dy) in enumerate(GROUPS):
        (xa, xb), (ya, yb) = TAKE[dx], TAKE[dy]
        x0, y0 = xa + CX * dx + 2, ya + CY * dy + 2
        columns[0:2] = recv_z_lo[g]
        columns[2:6] = recv_z_hi[g]
        ztile[:, :, :, 0:8] = columns[...].T.reshape(CX, 4, CY, 8)
        halo[x0 : x0 + xb - xa, :, y0 : y0 + yb - ya] = ztile[xa:xb, :, ya:yb]

    def interpolate(planes):
        first, count = PLACE[planes[0]], len(planes)
        span = count * WY
        rows = dot3(
            vel_h[:, first : first + count].reshape(3 * span, WZ),
            vel_l[:, first : first + count].reshape(3 * span, WZ),
            own_h[...], own_l[...], ((1,), (0,)),
        )
        starts = [STARTS[CENTRE] + (x - 1) * WY for x in planes]
        weight = jnp.concatenate([wxy[start : start + WY] for start in starts], axis=0)
        return [
            jnp.sum(rows[c * span : (c + 1) * span] * weight, axis=0, keepdims=True)
            for c in range(3)
        ]

    for x in range(1, 12):
        for c in range(3):
            high, low = split(widened(x, c))
            vel_h[c, PLACE[x]] = high
            vel_l[c, PLACE[x]] = low
    for c, value in enumerate(interpolate(OUTER + MIDDLE)):
        vecs[0, c : c + 1] = live * (target_ref[c : c + 1] - value)

    def send_vector(a):
        for dx, dy, dz in NEIGHBOURS:
            back = slot_of(-dx, -dy, -dz)
            remote(
                vecs.at[a], recv_v.at[a, back], send_v.at[a], got_v.at[a, abs(dx) + abs(dy) + abs(dz) - 1],
                at(dx, dy, dz),
            ).start()
        recv_v[a, slot_of(0, 0, 0)] = vecs[a]

    part_row = lax.broadcasted_iota(jnp.int32, (16, CAP), 0)

    def spread_inner(a, g):
        span = SPANS[g]
        vector = recv_v[a, 3 * g + 2]
        weight = wxy[STARTS[g] : STARTS[g] + span]
        for c in range(3):
            high, low = split(weight * vector[c : c + 1])
            left_h[c * span : (c + 1) * span] = high
            left_l[c * span : (c + 1) * span] = low
        return dot3(left_h[0 : 3 * span], left_l[0 : 3 * span], table_h[g], table_l[g], ((1,), (1,)))

    def spread_edges(a, g):
        rows = slice(STARTS[g], STARTS[g] + SPANS[g])
        sides = []
        for j in range(2):
            vector = recv_v[a, 3 * g + j]
            value = jnp.where(
                part_row < 4, vector[0:1], jnp.where(part_row < 8, vector[1:2], vector[2:3])
            )
            high, low = split(edge_w[2 * g + j] * value)
            sides.append(dot3(high, low, wxy_h[j, rows], wxy_l[j, rows], ((1,), (1,))))
        return jnp.concatenate(sides, axis=0).T

    def add_inner(a, g):
        (dx, dy), span = GROUPS[g], SPANS[g]
        x0, nx = PLANES[dx]
        y0, ny = ROWS[dy]
        total = spread_inner(a, g)
        for c in range(3):
            at_place = (c, slice(x0, x0 + nx), slice(y0, y0 + ny), slice(0, TZ))
            grid[at_place] += total[c * span : (c + 1) * span].reshape(nx, ny, TZ)

    def add_edges(a, g):
        dx, dy = GROUPS[g]
        x0, nx = PLANES[dx]
        y0, ny = ROWS[dy]
        edges[x0 : x0 + nx, y0 : y0 + ny, 0:32] += spread_edges(a, g).reshape(nx, ny, 32)

    def spread(a, middle):
        far = [abs(dx) + abs(dy) for dx, dy in GROUPS]
        grid[:, :, :, 0:TZ] = jnp.zeros((3, WX, WY, TZ), F32)
        edges[:, :, 0:32] = jnp.zeros((WX, WY, 32), F32)
        kept = None
        for hops, messages in enumerate((0, 6, 12, 8)):
            if hops:
                drain(recv_v.at[a, 0:messages], got_v.at[a, hops - 1])
            if hops == 3:
                kept = middle()
            for g in range(9):
                if far[g] == hops:
                    add_inner(a, g)
            for g in range(9):
                if far[g] == hops - 1:
                    add_edges(a, g)
        return kept

    def shifts(value, axis):
        length = value.shape[axis]
        return pltpu.roll(value, 1, axis), pltpu.roll(value, length - 1, axis)

    def both(value, axis):
        before, after = shifts(value, axis)
        return before + after

    def stream(last, planes, outputs, energy):
        inner = range(2, 10) if last else range(1, 12)
        for x in planes:
            scale = wide[x]
            edge = edges[x]
            values = []
            for c in range(3):
                head = grid[c, x, :, 0:CZ] + jnp.where(
                    lane < 4, pltpu.roll(edge, CZ - 4 * c, 1) if c else edge, 0.0
                )
                tail = grid[c, x, :, CZ:] + jnp.where(
                    (lane > 0) & (lane < 5), pltpu.roll(edge, CZ - 15 - 4 * c, 1), 0.0
                )
                values.append(scale * jnp.concatenate([head, tail], axis=1))
            m0, m1, m2 = values
            moved[0, x], moved[1, x], moved[2, x] = m0, m1, m2
            before, after = shifts(m0, 0)
            sy0, dy0 = before + after, before - after
            before, after = shifts(m1, 0)
            sy1, dy1 = before + after, before - after
            before, after = shifts(m0, 1)
            sz0, dz0 = before + after, before - after
            before, after = shifts(m2, 1)
            sz2, dz2 = before + after, before - after
            plane_a[0, x] = 2.0 * m0 + sy0 + sz0
            plane_b[0, x] = dy1 + dz2
            plane_a[1, x] = sy1
            plane_b[1, x] = dy0
            plane_a[2, x] = sz2
            plane_b[2, x] = dz0
            if x in inner:
                before, after = shifts(dz2, 0)
                plane_c[0, x] = 2.0 * sy1 + both(sy1, 1) + (before - after)
                before, after = shifts(dy1, 1)
                plane_c[1, x] = 2.0 * sz2 + both(sz2, 0) + (before - after)

        for x in outputs:
            half = wide[x] * 0.5
            for c in range(3):
                post = plane_a[c, x - 1] + plane_a[c, x + 1] + plane_b[c, x - 1] - plane_b[c, x + 1]
                if c:
                    post = post + plane_c[c - 1, x]
                response = moved[c, x] + post * (1.0 / 12.0)
                if last:
                    energy = energy + moved[c, x] * response
                else:
                    high, low = split(half * response)
                    vel_h[c, PLACE[x]] = high
                    vel_l[c, PLACE[x]] = low
        return energy

    lane_row = lax.broadcasted_iota(jnp.int32, (1, 128), 1)
    me = iy * size_z + iz
    mates = size_y * size_z - 1
    far_mates = [(y, z) for y in range(size_y) for z in range(size_z) if (y, z) != (0, 0)]
    far_mates.sort(key=lambda k: -(min(k[0], size_y - k[0]) / 2 + min(k[1], size_z - k[1])))

    def sum_plane(k, row):
        part[k] = row
        recv_a[k, me] = row
        for other in far_mates:
            remote(part.at[k], recv_a.at[k, me], send_r.at[k], got_r.at[k], mate(*other)).start()

    def sum_along(k):
        drain(recv_a.at[k, 0:mates], got_r.at[k])
        row = jnp.sum(recv_a[k], axis=0)
        part_b[k] = row
        recv_b[k, ix] = row
        for other in sorted(range(1, size_x), key=lambda k: -min(k, size_x - k)):
            remote(
                part_b.at[k], recv_b.at[k, ix], send_r.at[2 + k], got_r.at[2 + k], along(other)
            ).start()

    def summed(k):
        drain(recv_b.at[k, 0 : size_x - 1], got_r.at[2 + k])
        return jnp.sum(recv_b[k], axis=0)

    for a in range(ITERS):
        send_vector(a)
        if a == 0:
            for dx, dy in around:
                scale_copy(dx, dy).wait_recv()
            place(
                TAKE, (3,), field, lambda dx, planes, k: srecv_x[(dx + 1) // 2, planes],
                srecv_lo, srecv_hi, 0, 0,
            )
            for x in range(WX):
                wide[x] = widened(x, 3)
            drain(marks.at[0:26], got_m)
            for g in ORDER:
                for j in range(3):
                    if (g, j) != (CENTRE, 2):
                        build(g, j)
        last = a == ITERS - 1
        if last:
            v = [vecs[k, 0:3] for k in range(3)]
            w = [images[k, 0:3] for k in range(2)]
            pairs = [(v[0], w[0]), (v[0], w[1]), (v[2], w[0]), (v[1], w[1]), (v[2], w[1])]
            pairs = pairs + [(v[0], v[j]) for j in range(3)]
            row = jnp.zeros((1, 128), F32)
            for k, (left, right) in enumerate(pairs):
                row = jnp.where(lane_row == k, jnp.sum(left * right), row)
            sum_plane(0, row)

        def middle():
            energy = stream(last, range(4, 9), MIDDLE, jnp.zeros((WY, WZ), F32))
            return energy if last else interpolate(MIDDLE)

        kept = spread(a, middle)
        if last:
            sum_along(0)
            energy = stream(last, (1, 2, 3, 9, 10), (2, 3, 4, 8, 9), kept)
        else:
            stream(last, (0, 1, 2, 3, 9, 10, 11, 12), OUTER, None)
            for c, value in enumerate(interpolate(OUTER)):
                vector = vecs[a, c : c + 1]
                image = live * (kept[c] + value + stiff * vector)
                images[a, c : c + 1] = image
                vecs[a + 1, c : c + 1] = image - SHIFT * vector

    inside = lambda axis, size: (
        lax.broadcasted_iota(jnp.int32, (WY, WZ), axis) - 2
    ).astype(jnp.uint32) < size
    energy = jnp.where(inside(0, CY) & inside(1, CZ), energy, 0.0)
    own = jnp.sum(0.5 * energy, axis=0, keepdims=True)
    own = own + jnp.sum(stiff * v[2] * v[2], axis=0, keepdims=True)
    sum_plane(1, own[:, 0:128] + own[:, 128:256])
    total = summed(0)
    h00, h01, h02, h11, h12, b0, b1, b2 = (
        jnp.sum(jnp.where(lane_row == k, total, 0.0), axis=1, keepdims=True) for k in range(8)
    )

    def over(top, pivot, size):
        fine = pivot > 1e-7 * size
        return jnp.where(fine, top / jnp.where(fine, pivot, 1.0), 0.0)

    l10 = over(h01, h00, h00)
    l20 = over(h02, h00, h00)
    d1 = h11 - l10 * h01
    e12 = h12 - l10 * h02
    l21 = over(e12, d1, h11)
    less = h02 * l20 + l21 * e12
    z1 = b1 - l10 * b0
    z2 = b2 - l20 * b0 - l21 * z1
    y1 = over(z1, d1, h11)
    y0 = over(b0, h00, h00) - l10 * y1
    first = y0 * v[0] + y1 * v[1]
    second = v[2] - l21 * v[1] + (l10 * l21 - l20) * v[0]
    sum_along(1)
    h22 = jnp.sum(summed(1), axis=1, keepdims=True)
    out_ref[...] = first + over(z2, h22 - less, h22) * second

    for dx, dy in GROUPS:
        if (dx, dy) != (0, 0):
            halo_copy(dx, dy).wait_send()
            scale_copy(dx, dy).wait_send()
    drain(recv_z_lo.at[0:6], send_z.at[0])
    drain(recv_z_hi.at[0:6], send_z.at[1])
    drain(marks.at[0:26], send_m)
    for a in range(ITERS):
        drain(recv_v.at[a, 0:26], send_v.at[a])
    for k in range(2):
        drain(recv_a.at[k, 0:mates], send_r.at[k])
        drain(recv_b.at[k, 0 : size_x - 1], send_r.at[2 + k])


def solution(mesh):
    sizes = tuple(mesh.shape[a] for a in AXES)
    plane = sizes[1] * sizes[2]

    def body(density, base_velocity, cells, offsets, target, stiffness, counts):
        vmem = pl.BlockSpec(memory_space=pltpu.VMEM)
        return pl.pallas_call(
            functools.partial(kernel, sizes),
            out_shape=jax.ShapeDtypeStruct((3, CAP), F32),
            in_specs=[pl.BlockSpec(memory_space=pl.ANY)] * 7,
            out_specs=vmem,
            scratch_shapes=[
                pltpu.SMEM((1,), jnp.int32),
                pltpu.VMEM((CX, CY, CZ), F32),
                pltpu.VMEM((3, CAP), jnp.int32),
                pltpu.VMEM((3, CAP), F32),
                pltpu.VMEM((3, CAP), F32),
                pltpu.VMEM((1, CAP), F32),
                pltpu.VMEM((CX, 4, CY, CZ), F32),
                pltpu.VMEM((CZ, 4 * CX * CY), F32),
                pltpu.VMEM((CX, 4, CZ), F32),
                pltpu.VMEM((CX, 8, CZ), F32),
                pltpu.VMEM((CX, 2, CZ), F32),
                pltpu.VMEM((CX, 4, CZ), F32),
                pltpu.VMEM((2, 4 * CX * CY), F32),
                pltpu.VMEM((4, 4 * CX * CY), F32),
                pltpu.VMEM((8, CAP), F32),
                pltpu.VMEM((2, CX, 3, CY, CZ), F32),
                pltpu.VMEM((3, CX, 4, CZ), F32),
                pltpu.VMEM((3, CX, 8, CZ), F32),
                pltpu.VMEM((2, CX, CY, CZ), F32),
                pltpu.VMEM((3, CX, 2, CZ), F32),
                pltpu.VMEM((3, CX, 4, CZ), F32),
                pltpu.VMEM((9, 2, 4 * CX * CY), F32),
                pltpu.VMEM((9, 4, 4 * CX * CY), F32),
                pltpu.VMEM((8, 4 * CX * CY), F32),
                pltpu.VMEM((27, 8, CAP), F32),
                pltpu.VMEM((WX, 4, WY, CZ), F32),
                pltpu.VMEM((WX, 4, WY, CZ), F32),
                pltpu.VMEM((CX, 4, CY, CZ), F32),
                pltpu.VMEM((WX, WY, WZ), F32),
                pltpu.VMEM((9, TZ, CAP), BF16),
                pltpu.VMEM((9, TZ, CAP), BF16),
                pltpu.VMEM((WZ, CAP), BF16),
                pltpu.VMEM((WZ, CAP), BF16),
                pltpu.VMEM((sum(SPANS), CAP), F32),
                pltpu.VMEM((2, sum(SPANS), CAP), BF16),
                pltpu.VMEM((2, sum(SPANS), CAP), BF16),
                pltpu.VMEM((18, 16, CAP), F32),
                pltpu.VMEM((3 * max(SPANS), CAP), BF16),
                pltpu.VMEM((3 * max(SPANS), CAP), BF16),
                pltpu.VMEM((3, WX, WY, WZ), F32),
                pltpu.VMEM((WX, WY, CZ), F32),
                pltpu.VMEM((3, WX, WY, WZ), F32),
                pltpu.VMEM((3, WX, WY, WZ), F32),
                pltpu.VMEM((3, WX, WY, WZ), F32),
                pltpu.VMEM((2, WX, WY, WZ), F32),
                pltpu.VMEM((3, 11, WY, WZ), BF16),
                pltpu.VMEM((3, 11, WY, WZ), BF16),
                pltpu.VMEM((ITERS + 1, 4, CAP), F32),
                pltpu.VMEM((ITERS, 4, CAP), F32),
                pltpu.VMEM((ITERS, 27, 4, CAP), F32),
                pltpu.VMEM((2, 1, 128), F32),
                pltpu.VMEM((2, plane, 1, 128), F32),
                pltpu.VMEM((2, 1, 128), F32),
                pltpu.VMEM((2, sizes[0], 1, 128), F32),
                pltpu.SemaphoreType.DMA((9,)),
                pltpu.SemaphoreType.DMA((9,)),
                pltpu.SemaphoreType.DMA((9,)),
                pltpu.SemaphoreType.DMA((9,)),
                pltpu.SemaphoreType.DMA((9,)),
                pltpu.SemaphoreType.DMA((2,)),
                pltpu.SemaphoreType.DMA((2,)),
                pltpu.SemaphoreType.DMA,
                pltpu.SemaphoreType.DMA,
                pltpu.SemaphoreType.DMA((ITERS,)),
                pltpu.SemaphoreType.DMA((ITERS, 3)),
                pltpu.SemaphoreType.DMA((4,)),
                pltpu.SemaphoreType.DMA((4,)),
            ],
            compiler_params=pltpu.CompilerParams(
                collective_id=0, has_side_effects=True, vmem_limit_bytes=60 * 1024 * 1024
            ),
            name="immersed",
        )(density, base_velocity, cells, offsets, target, stiffness[None], counts)

    return jax.shard_map(
        body,
        mesh=mesh,
        in_specs=(
            P(*AXES), P(None, *AXES), P(None, ALL), P(None, ALL), P(None, ALL), P(ALL), P(ALL),
        ),
        out_specs=P(None, ALL),
        check_vma=False,
    )
```

```python
import functools

import jax
import jax.numpy as jnp
from jax import lax
from jax.experimental import pallas as pl
from jax.experimental.pallas import tpu as pltpu
from jax.sharding import PartitionSpec as P

ITERS = 3
CX, CY, CZ = 8, 8, 128
CAP = 256
WX, WY, WZ = 13, 16, 256
TZ = 144
AXES = ("gx", "gy", "gz")
ALL = ("gx", "gy", "gz")
MESH = pl.DeviceIdType.MESH
SHIFT = 0.1
F32, BF16 = jnp.float32, jnp.bfloat16

GROUPS = [(dx, dy) for dx in (-1, 0, 1) for dy in (-1, 0, 1)]
DZS = (-1, 1, 0)
ORDER = sorted(range(9), key=lambda g: abs(GROUPS[g][0]) + abs(GROUPS[g][1]))
PLANES = {-1: (0, 4), 0: (1, 12), 1: (9, 4)}
ROWS = {-1: (0, 8), 0: (0, 16), 1: (8, 8)}
TAKE = {-1: (6, 8), 0: (0, 8), 1: (0, 3)}
TAKE_BASE = {-1: (7, 8), 0: (0, 8), 1: (0, 2)}
MIDDLE = (5, 6, 7)
OUTER = (1, 2, 3, 4, 8, 9, 10, 11)
PLACE = {x: k for k, x in enumerate(OUTER + MIDDLE)}


def group_of(dx, dy):
    return (dx + 1) * 3 + dy + 1


def slot_of(dx, dy, dz):
    return group_of(dx, dy) * 3 + DZS.index(dz)


NEIGHBOURS = [
    (GROUPS[g][0], GROUPS[g][1], dz)
    for g in ORDER
    for dz in DZS
    if (GROUPS[g][0], GROUPS[g][1], dz) != (0, 0, 0)
]
NEIGHBOURS.sort(key=lambda offset: sum(map(abs, offset)))
CENTRE = group_of(0, 0)
SPANS = [PLANES[dx][1] * ROWS[dy][1] for dx, dy in GROUPS]
STARTS = [sum(SPANS[:g]) for g in range(9)]


def split(value):
    high = value.astype(BF16)
    return high, (value - high.astype(F32)).astype(BF16)


def dot3(lh, ll, rh, rl, dims):
    dot = functools.partial(
        lax.dot_general, dimension_numbers=(dims, ((), ())), preferred_element_type=F32
    )
    count = lh.shape[0]
    both = dot(jnp.concatenate([lh, ll], axis=0), rh)
    return both[:count] + (both[count:] + dot(lh, rl))


def kernel(
    sizes,
    density_in, base_in, cells_in, offsets_in, target_in, stiff_in, counts_in,
    out_ref,
    counts_ref,
    density_ref, cells_ref, offsets_ref, target_ref, stiff_ref,
    field, ftrans, pack_lo, pack_hi, spack_lo, spack_hi, pack_z_lo, pack_z_hi, mark_own,
    recv_x, recv_lo, recv_hi, srecv_x, srecv_lo, srecv_hi,
    recv_z_lo, recv_z_hi, columns, marks, main, halo, ztile, wide,
    table_h, table_l, own_h, own_l, wxy, wxy_h, wxy_l, edge_w, left_h, left_l, grid, edges, moved, plane_a, plane_b, plane_c,
    vel_h, vel_l, vecs, images, recv_v, part, recv_a, part_b, recv_b,
    loaded, send_f, got_f, send_s, got_s, send_z, got_z, send_m, got_m, send_v, got_v, send_r, got_r,
):
    size_x, size_y, size_z = sizes
    ix, iy, iz = (lax.axis_index(a) for a in AXES)

    def at(dx, dy, dz):
        return (
            lax.rem(ix + dx + size_x, size_x),
            lax.rem(iy + dy + size_y, size_y),
            lax.rem(iz + dz + size_z, size_z),
        )

    def mate(y, z):
        return (ix, lax.rem(iy + y, size_y), lax.rem(iz + z, size_z))

    def along(k):
        return (lax.rem(ix + k, size_x), iy, iz)

    loads = [
        pltpu.make_async_copy(base_in.at[c], field.at[:, c], loaded.at[c]) for c in range(3)
    ]
    loads += [
        pltpu.make_async_copy(source, target, loaded.at[3 + k])
        for k, (source, target) in enumerate(
            [
                (density_in, density_ref), (cells_in, cells_ref), (offsets_in, offsets_ref),
                (target_in, target_ref), (stiff_in, stiff_ref), (counts_in, counts_ref),
            ]
        )
    ]
    for load in loads:
        load.start()

    barrier = pltpu.get_barrier_semaphore()
    for offset in reversed(NEIGHBOURS):
        pl.semaphore_signal(barrier, inc=1, device_id=at(*offset), device_id_type=MESH)

    for load in loads[0:4]:
        load.wait()
    field[:, 3] = lax.rsqrt(density_ref[...])
    ftrans[...] = field[...].reshape(4 * CX * CY, CZ).T
    pack_z_lo[...] = ftrans[CZ - 2 : CZ]
    pack_z_hi[...] = ftrans[0:4]
    for c in range(3):
        pack_lo[:, c : c + 1] = field[:, c, CY - 1 : CY]
        pack_hi[:, 2 * c : 2 * c + 2] = field[:, c, 0:2]
    spack_lo[...] = field[:, 3, CY - 2 : CY]
    spack_hi[...] = field[:, 3, 0:4]
    for load in loads[4:]:
        load.wait()
    anchors = (ix * CX, iy * CY, iz * CZ)
    for k in range(3):
        mark_own[k : k + 1] = (cells_ref[k : k + 1] - anchors[k]).astype(F32)
    mark_own[3:6] = offsets_ref[...]
    mark_own[6:8] = jnp.zeros((2, CAP), F32)
    marks[slot_of(0, 0, 0)] = mark_own[...]

    pl.semaphore_wait(barrier, len(NEIGHBOURS))

    def remote(src, dst, send, recv, device):
        return pltpu.make_async_remote_copy(
            src_ref=src, dst_ref=dst, send_sem=send, recv_sem=recv, device_id=device,
            device_id_type=MESH,
        )

    def drain(ref, sem):
        pltpu.make_async_copy(ref, ref, sem).wait()

    def halo_copy(dx, dy):
        a, b = TAKE_BASE[-dx]
        g = group_of(-dx, -dy)
        if dy == 0:
            pair = field.at[a:b, 0:3], recv_x.at[(1 - dx) // 2, a:b]
        elif dy == 1:
            pair = pack_lo.at[a:b], recv_lo.at[1 - dx, a:b]
        else:
            pair = pack_hi.at[a:b], recv_hi.at[1 - dx, a:b]
        return remote(*pair, send_f.at[g], got_f.at[g], at(dx, dy, 0))

    def scale_copy(dx, dy):
        a, b = TAKE[-dx]
        g = group_of(-dx, -dy)
        if dy == 0:
            pair = field.at[a:b, 3], srecv_x.at[(1 - dx) // 2, a:b]
        elif dy == 1:
            pair = spack_lo.at[a:b], srecv_lo.at[1 - dx, a:b]
        else:
            pair = spack_hi.at[a:b], srecv_hi.at[1 - dx, a:b]
        return remote(*pair, send_s.at[g], got_s.at[g], at(dx, dy, 0))

    def edge_copy(dx, dy, dz):
        a, b = {-1: (0, 128), 0: (0, 256), 1: (128, 256)}[dx]
        g = group_of(-dx, -dy)
        if dz == 1:
            pair = pack_z_lo.at[:, a:b], recv_z_lo.at[g, :, a:b]
        else:
            pair = pack_z_hi.at[:, a:b], recv_z_hi.at[g, :, a:b]
        side = (1 - dz) // 2
        return remote(*pair, send_z.at[side], got_z.at[side], at(dx, dy, dz))

    around = [GROUPS[g] for g in reversed(ORDER) if g != CENTRE]
    for dx, dy, dz in NEIGHBOURS:
        if dz:
            edge_copy(dx, dy, dz).start()
    for dx, dy in around:
        halo_copy(dx, dy).start()
    for dx, dy in around:
        scale_copy(dx, dy).start()
    for dx, dy, dz in NEIGHBOURS:
        back = slot_of(-dx, -dy, -dz)
        remote(mark_own, marks.at[back], send_m, got_m, at(dx, dy, dz)).start()

    own_h[...] = jnp.zeros(own_h.shape, BF16)
    own_l[...] = jnp.zeros(own_l.shape, BF16)
    ztile[...] = jnp.zeros(ztile.shape, F32)
    columns[...] = jnp.zeros(columns.shape, F32)
    main[...] = jnp.zeros(main.shape, F32)
    halo[:, :, 8:16] = jnp.zeros((WX, 4, 8, CZ), F32)
    grid[...] = jnp.zeros(grid.shape, F32)
    edges[...] = jnp.zeros(edges.shape, F32)
    vecs[...] = jnp.zeros(vecs.shape, F32)

    live = (lax.broadcasted_iota(jnp.int32, (1, CAP), 1) < counts_ref[0]).astype(F32)
    stiff = stiff_ref[...]

    def axis_table(first, rows, start, weights):
        away = (
            lax.broadcasted_iota(jnp.int32, (rows, CAP), 0).astype(F32) + float(first) - start
        )
        value = jnp.zeros((rows, CAP), F32)
        for step in range(4):
            value = jnp.where(away == float(step), weights[step], value)
        return value

    def build(g, j):
        (dx, dy), dz = GROUPS[g], DZS[j]
        mark = marks[g * 3 + j]
        fraction = mark[3:6]
        root = jnp.sqrt(1.0 + 4.0 * fraction - 4.0 * fraction * fraction)
        weights = [
            (3.0 - 2.0 * fraction - root) * 0.125,
            (3.0 - 2.0 * fraction + root) * 0.125,
            (1.0 + 2.0 * fraction + root) * 0.125,
            (1.0 + 2.0 * fraction - root) * 0.125,
        ]
        of = lambda k: [w[k : k + 1] for w in weights]
        x0, nx = PLANES[dx]
        y0, ny = ROWS[dy]
        table_x = axis_table(x0, 16, mark[0:1] + float(1 + CX * dx), of(0))
        table_y = axis_table(y0, ny, mark[1:2] + float(1 + CY * dy), of(1))
        for x in range(nx):
            rows = slice(STARTS[g] + x * ny, STARTS[g] + (x + 1) * ny)
            weight = table_x[x : x + 1] * table_y
            if dz == 0:
                wxy[rows] = weight
            else:
                high, low = split(weight)
                wxy_h[j, rows] = high
                wxy_l[j, rows] = low
        start = mark[2:3] + float(1 + CZ * dz)
        if dz == 0:
            high, low = split(axis_table(0, TZ, start, of(2)))
            table_h[g] = high
            table_l[g] = low
            if g == CENTRE:
                own_h[0:TZ] = high
                own_l[0:TZ] = low
        else:
            touched = axis_table({-1: 0, 1: CZ + 1}[dz], 8, start, of(2))[0:4]
            edge_w[2 * g + j, 0:12] = jnp.concatenate([touched] * 3, axis=0)
            edge_w[2 * g + j, 12:16] = jnp.zeros((4, CAP), F32)

    build(CENTRE, 2)

    lane = lax.broadcasted_iota(jnp.int32, (WY, CZ), 1)

    def place(takes, comps, centre, sides, low, high, low_step, high_step):
        for g, (dx, dy) in enumerate(GROUPS):
            (xa, xb), (ya, yb) = takes[dx], takes[dy]
            x0, y0 = xa + CX * dx + 2, ya + CY * dy + 2
            planes, rows = slice(x0, x0 + xb - xa), slice(y0, y0 + yb - ya)
            for k, c in enumerate(comps):
                if g == CENTRE:
                    main[planes, c, rows] = centre[:, c]
                elif dy == 0:
                    main[planes, c, rows] = sides(dx, slice(xa, xb), k)
                elif dy == -1:
                    first = k * low_step
                    main[planes, c, rows] = low[dx + 1, xa:xb, first : first + yb - ya]
                else:
                    first = k * high_step
                    main[planes, c, rows] = high[dx + 1, xa:xb, first : first + yb - ya]

    def widened(x, c):
        turned = pltpu.roll(main[x, c], 2, 1)
        edge = halo[x, c]
        head = jnp.where(lane < 2, edge, turned)
        tail = jnp.where(lane < 2, turned, jnp.where(lane < 5, edge, 0.0))
        return jnp.concatenate([head, tail], axis=1)

    for dx, dy in around:
        halo_copy(dx, dy).wait_recv()
    place(
        TAKE_BASE, (0, 1, 2), field, lambda dx, planes, k: recv_x[(dx + 1) // 2, planes, k],
        recv_lo, recv_hi, 1, 2,
    )
    drain(recv_z_lo.at[0:6], got_z.at[0])
    drain(recv_z_hi.at[0:6], got_z.at[1])
    for g, (dx, dy) in enumerate(GROUPS):
        (xa, xb), (ya, yb) = TAKE[dx], TAKE[dy]
        x0, y0 = xa + CX * dx + 2, ya + CY * dy + 2
        columns[0:2] = recv_z_lo[g]
        columns[2:6] = recv_z_hi[g]
        ztile[:, :, :, 0:8] = columns[...].T.reshape(CX, 4, CY, 8)
        halo[x0 : x0 + xb - xa, :, y0 : y0 + yb - ya] = ztile[xa:xb, :, ya:yb]

    def interpolate(planes):
        first, count = PLACE[planes[0]], len(planes)
        span = count * WY
        rows = dot3(
            vel_h[:, first : first + count].reshape(3 * span, WZ),
            vel_l[:, first : first + count].reshape(3 * span, WZ),
            own_h[...], own_l[...], ((1,), (0,)),
        )
        starts = [STARTS[CENTRE] + (x - 1) * WY for x in planes]
        weight = jnp.concatenate([wxy[start : start + WY] for start in starts], axis=0)
        return [
            jnp.sum(rows[c * span : (c + 1) * span] * weight, axis=0, keepdims=True)
            for c in range(3)
        ]

    for x in range(1, 12):
        for c in range(3):
            high, low = split(widened(x, c))
            vel_h[c, PLACE[x]] = high
            vel_l[c, PLACE[x]] = low
    for c, value in enumerate(interpolate(OUTER + MIDDLE)):
        vecs[0, c : c + 1] = live * (target_ref[c : c + 1] - value)

    def send_vector(a):
        for dx, dy, dz in NEIGHBOURS:
            back = slot_of(-dx, -dy, -dz)
            remote(
                vecs.at[a], recv_v.at[a, back], send_v.at[a], got_v.at[a, abs(dx) + abs(dy) + abs(dz) - 1],
                at(dx, dy, dz),
            ).start()
        recv_v[a, slot_of(0, 0, 0)] = vecs[a]

    part_row = lax.broadcasted_iota(jnp.int32, (16, CAP), 0)

    def spread_inner(a, g):
        span = SPANS[g]
        vector = recv_v[a, 3 * g + 2]
        weight = wxy[STARTS[g] : STARTS[g] + span]
        for c in range(3):
            high, low = split(weight * vector[c : c + 1])
            left_h[c * span : (c + 1) * span] = high
            left_l[c * span : (c + 1) * span] = low
        return dot3(left_h[0 : 3 * span], left_l[0 : 3 * span], table_h[g], table_l[g], ((1,), (1,)))

    def spread_edges(a, g):
        rows = slice(STARTS[g], STARTS[g] + SPANS[g])
        sides = []
        for j in range(2):
            vector = recv_v[a, 3 * g + j]
            value = jnp.where(
                part_row < 4, vector[0:1], jnp.where(part_row < 8, vector[1:2], vector[2:3])
            )
            high, low = split(edge_w[2 * g + j] * value)
            sides.append(dot3(high, low, wxy_h[j, rows], wxy_l[j, rows], ((1,), (1,))))
        return jnp.concatenate(sides, axis=0).T

    def add_inner(a, g):
        (dx, dy), span = GROUPS[g], SPANS[g]
        x0, nx = PLANES[dx]
        y0, ny = ROWS[dy]
        total = spread_inner(a, g)
        for c in range(3):
            at_place = (c, slice(x0, x0 + nx), slice(y0, y0 + ny), slice(0, TZ))
            grid[at_place] += total[c * span : (c + 1) * span].reshape(nx, ny, TZ)

    def add_edges(a, g):
        dx, dy = GROUPS[g]
        x0, nx = PLANES[dx]
        y0, ny = ROWS[dy]
        edges[x0 : x0 + nx, y0 : y0 + ny, 0:32] += spread_edges(a, g).reshape(nx, ny, 32)

    def spread(a, middle):
        far = [abs(dx) + abs(dy) for dx, dy in GROUPS]
        grid[:, :, :, 0:TZ] = jnp.zeros((3, WX, WY, TZ), F32)
        edges[:, :, 0:32] = jnp.zeros((WX, WY, 32), F32)
        kept = None
        for hops, messages in enumerate((0, 6, 12, 8)):
            if hops:
                drain(recv_v.at[a, 0:messages], got_v.at[a, hops - 1])
            if hops == 3:
                kept = middle()
            for g in range(9):
                if far[g] == hops:
                    add_inner(a, g)
            for g in range(9):
                if far[g] == hops - 1:
                    add_edges(a, g)
        return kept

    def shifts(value, axis):
        length = value.shape[axis]
        return pltpu.roll(value, 1, axis), pltpu.roll(value, length - 1, axis)

    def both(value, axis):
        before, after = shifts(value, axis)
        return before + after

    def stream(last, planes, outputs, energy):
        inner = range(2, 10) if last else range(1, 12)
        for x in planes:
            scale = wide[x]
            edge = edges[x]
            values = []
            for c in range(3):
                head = grid[c, x, :, 0:CZ] + jnp.where(
                    lane < 4, pltpu.roll(edge, CZ - 4 * c, 1) if c else edge, 0.0
                )
                tail = grid[c, x, :, CZ:] + jnp.where(
                    (lane > 0) & (lane < 5), pltpu.roll(edge, CZ - 15 - 4 * c, 1), 0.0
                )
                values.append(scale * jnp.concatenate([head, tail], axis=1))
            m0, m1, m2 = values
            moved[0, x], moved[1, x], moved[2, x] = m0, m1, m2
            before, after = shifts(m0, 0)
            sy0, dy0 = before + after, before - after
            before, after = shifts(m1, 0)
            sy1, dy1 = before + after, before - after
            before, after = shifts(m0, 1)
            sz0, dz0 = before + after, before - after
            before, after = shifts(m2, 1)
            sz2, dz2 = before + after, before - after
            plane_a[0, x] = 2.0 * m0 + sy0 + sz0
            plane_b[0, x] = dy1 + dz2
            plane_a[1, x] = sy1
            plane_b[1, x] = dy0
            plane_a[2, x] = sz2
            plane_b[2, x] = dz0
            if x in inner:
                before, after = shifts(dz2, 0)
                plane_c[0, x] = 2.0 * sy1 + both(sy1, 1) + (before - after)
                before, after = shifts(dy1, 1)
                plane_c[1, x] = 2.0 * sz2 + both(sz2, 0) + (before - after)

        for x in outputs:
            half = wide[x] * 0.5
            for c in range(3):
                post = plane_a[c, x - 1] + plane_a[c, x + 1] + plane_b[c, x - 1] - plane_b[c, x + 1]
                if c:
                    post = post + plane_c[c - 1, x]
                response = moved[c, x] + post * (1.0 / 12.0)
                if last:
                    energy = energy + moved[c, x] * response
                else:
                    high, low = split(half * response)
                    vel_h[c, PLACE[x]] = high
                    vel_l[c, PLACE[x]] = low
        return energy

    lane_row = lax.broadcasted_iota(jnp.int32, (1, 128), 1)
    me = iy * size_z + iz
    mates = size_y * size_z - 1
    far_mates = [(y, z) for y in range(size_y) for z in range(size_z) if (y, z) != (0, 0)]
    far_mates.sort(key=lambda k: -(min(k[0], size_y - k[0]) / 2 + min(k[1], size_z - k[1])))

    def sum_plane(k, row):
        part[k] = row
        recv_a[k, me] = row
        for other in far_mates:
            remote(part.at[k], recv_a.at[k, me], send_r.at[k], got_r.at[k], mate(*other)).start()

    def sum_along(k):
        drain(recv_a.at[k, 0:mates], got_r.at[k])
        row = jnp.sum(recv_a[k], axis=0)
        part_b[k] = row
        recv_b[k, ix] = row
        for other in sorted(range(1, size_x), key=lambda k: -min(k, size_x - k)):
            remote(
                part_b.at[k], recv_b.at[k, ix], send_r.at[2 + k], got_r.at[2 + k], along(other)
            ).start()

    def summed(k):
        drain(recv_b.at[k, 0 : size_x - 1], got_r.at[2 + k])
        return jnp.sum(recv_b[k], axis=0)

    for a in range(ITERS):
        send_vector(a)
        if a == 0:
            for dx, dy in around:
                scale_copy(dx, dy).wait_recv()
            place(
                TAKE, (3,), field, lambda dx, planes, k: srecv_x[(dx + 1) // 2, planes],
                srecv_lo, srecv_hi, 0, 0,
            )
            for x in range(WX):
                wide[x] = widened(x, 3)
            drain(marks.at[0:26], got_m)
            for g in ORDER:
                for j in range(3):
                    if (g, j) != (CENTRE, 2):
                        build(g, j)
        last = a == ITERS - 1
        if last:
            v = [vecs[k, 0:3] for k in range(3)]
            w = [images[k, 0:3] for k in range(2)]
            pairs = [(v[0], w[0]), (v[0], w[1]), (v[2], w[0]), (v[1], w[1]), (v[2], w[1])]
            pairs = pairs + [(v[0], v[j]) for j in range(3)]
            row = jnp.zeros((1, 128), F32)
            for k, (left, right) in enumerate(pairs):
                row = jnp.where(lane_row == k, jnp.sum(left * right), row)
            sum_plane(0, row)

        def middle():
            return None

        kept = spread(a, middle)
        if last:
            sum_along(0)
            energy = stream(last, range(1, 11), range(2, 10), jnp.zeros((WY, WZ), F32))
        else:
            stream(last, range(WX), range(1, 12), None)
            for c, value in enumerate(interpolate(OUTER + MIDDLE)):
                vector = vecs[a, c : c + 1]
                image = live * (value + stiff * vector)
                images[a, c : c + 1] = image
                vecs[a + 1, c : c + 1] = image - SHIFT * vector

    inside = lambda axis, size: (
        lax.broadcasted_iota(jnp.int32, (WY, WZ), axis) - 2
    ).astype(jnp.uint32) < size
    energy = jnp.where(inside(0, CY) & inside(1, CZ), energy, 0.0)
    own = jnp.sum(0.5 * energy, axis=0, keepdims=True)
    own = own + jnp.sum(stiff * v[2] * v[2], axis=0, keepdims=True)
    sum_plane(1, own[:, 0:128] + own[:, 128:256])
    total = summed(0)
    h00, h01, h02, h11, h12, b0, b1, b2 = (
        jnp.sum(jnp.where(lane_row == k, total, 0.0), axis=1, keepdims=True) for k in range(8)
    )

    def over(top, pivot, size):
        fine = pivot > 1e-7 * size
        return jnp.where(fine, top / jnp.where(fine, pivot, 1.0), 0.0)

    l10 = over(h01, h00, h00)
    l20 = over(h02, h00, h00)
    d1 = h11 - l10 * h01
    e12 = h12 - l10 * h02
    l21 = over(e12, d1, h11)
    less = h02 * l20 + l21 * e12
    z1 = b1 - l10 * b0
    z2 = b2 - l20 * b0 - l21 * z1
    y1 = over(z1, d1, h11)
    y0 = over(b0, h00, h00) - l10 * y1
    first = y0 * v[0] + y1 * v[1]
    second = v[2] - l21 * v[1] + (l10 * l21 - l20) * v[0]
    sum_along(1)
    h22 = jnp.sum(summed(1), axis=1, keepdims=True)
    out_ref[...] = first + over(z2, h22 - less, h22) * second

    for dx, dy in GROUPS:
        if (dx, dy) != (0, 0):
            halo_copy(dx, dy).wait_send()
            scale_copy(dx, dy).wait_send()
    drain(recv_z_lo.at[0:6], send_z.at[0])
    drain(recv_z_hi.at[0:6], send_z.at[1])
    drain(marks.at[0:26], send_m)
    for a in range(ITERS):
        drain(recv_v.at[a, 0:26], send_v.at[a])
    for k in range(2):
        drain(recv_a.at[k, 0:mates], send_r.at[k])
        drain(recv_b.at[k, 0 : size_x - 1], send_r.at[2 + k])


def solution(mesh):
    sizes = tuple(mesh.shape[a] for a in AXES)
    plane = sizes[1] * sizes[2]

    def body(density, base_velocity, cells, offsets, target, stiffness, counts):
        vmem = pl.BlockSpec(memory_space=pltpu.VMEM)
        return pl.pallas_call(
            functools.partial(kernel, sizes),
            out_shape=jax.ShapeDtypeStruct((3, CAP), F32),
            in_specs=[pl.BlockSpec(memory_space=pl.ANY)] * 7,
            out_specs=vmem,
            scratch_shapes=[
                pltpu.SMEM((1,), jnp.int32),
                pltpu.VMEM((CX, CY, CZ), F32),
                pltpu.VMEM((3, CAP), jnp.int32),
                pltpu.VMEM((3, CAP), F32),
                pltpu.VMEM((3, CAP), F32),
                pltpu.VMEM((1, CAP), F32),
                pltpu.VMEM((CX, 4, CY, CZ), F32),
                pltpu.VMEM((CZ, 4 * CX * CY), F32),
                pltpu.VMEM((CX, 4, CZ), F32),
                pltpu.VMEM((CX, 8, CZ), F32),
                pltpu.VMEM((CX, 2, CZ), F32),
                pltpu.VMEM((CX, 4, CZ), F32),
                pltpu.VMEM((2, 4 * CX * CY), F32),
                pltpu.VMEM((4, 4 * CX * CY), F32),
                pltpu.VMEM((8, CAP), F32),
                pltpu.VMEM((2, CX, 3, CY, CZ), F32),
                pltpu.VMEM((3, CX, 4, CZ), F32),
                pltpu.VMEM((3, CX, 8, CZ), F32),
                pltpu.VMEM((2, CX, CY, CZ), F32),
                pltpu.VMEM((3, CX, 2, CZ), F32),
                pltpu.VMEM((3, CX, 4, CZ), F32),
                pltpu.VMEM((9, 2, 4 * CX * CY), F32),
                pltpu.VMEM((9, 4, 4 * CX * CY), F32),
                pltpu.VMEM((8, 4 * CX * CY), F32),
                pltpu.VMEM((27, 8, CAP), F32),
                pltpu.VMEM((WX, 4, WY, CZ), F32),
                pltpu.VMEM((WX, 4, WY, CZ), F32),
                pltpu.VMEM((CX, 4, CY, CZ), F32),
                pltpu.VMEM((WX, WY, WZ), F32),
                pltpu.VMEM((9, TZ, CAP), BF16),
                pltpu.VMEM((9, TZ, CAP), BF16),
                pltpu.VMEM((WZ, CAP), BF16),
                pltpu.VMEM((WZ, CAP), BF16),
                pltpu.VMEM((sum(SPANS), CAP), F32),
                pltpu.VMEM((2, sum(SPANS), CAP), BF16),
                pltpu.VMEM((2, sum(SPANS), CAP), BF16),
                pltpu.VMEM((18, 16, CAP), F32),
                pltpu.VMEM((3 * max(SPANS), CAP), BF16),
                pltpu.VMEM((3 * max(SPANS), CAP), BF16),
                pltpu.VMEM((3, WX, WY, WZ), F32),
                pltpu.VMEM((WX, WY, CZ), F32),
                pltpu.VMEM((3, WX, WY, WZ), F32),
                pltpu.VMEM((3, WX, WY, WZ), F32),
                pltpu.VMEM((3, WX, WY, WZ), F32),
                pltpu.VMEM((2, WX, WY, WZ), F32),
                pltpu.VMEM((3, 11, WY, WZ), BF16),
                pltpu.VMEM((3, 11, WY, WZ), BF16),
                pltpu.VMEM((ITERS + 1, 4, CAP), F32),
                pltpu.VMEM((ITERS, 4, CAP), F32),
                pltpu.VMEM((ITERS, 27, 4, CAP), F32),
                pltpu.VMEM((2, 1, 128), F32),
                pltpu.VMEM((2, plane, 1, 128), F32),
                pltpu.VMEM((2, 1, 128), F32),
                pltpu.VMEM((2, sizes[0], 1, 128), F32),
                pltpu.SemaphoreType.DMA((9,)),
                pltpu.SemaphoreType.DMA((9,)),
                pltpu.SemaphoreType.DMA((9,)),
                pltpu.SemaphoreType.DMA((9,)),
                pltpu.SemaphoreType.DMA((9,)),
                pltpu.SemaphoreType.DMA((2,)),
                pltpu.SemaphoreType.DMA((2,)),
                pltpu.SemaphoreType.DMA,
                pltpu.SemaphoreType.DMA,
                pltpu.SemaphoreType.DMA((ITERS,)),
                pltpu.SemaphoreType.DMA((ITERS, 3)),
                pltpu.SemaphoreType.DMA((4,)),
                pltpu.SemaphoreType.DMA((4,)),
            ],
            compiler_params=pltpu.CompilerParams(
                collective_id=0, has_side_effects=True, vmem_limit_bytes=60 * 1024 * 1024
            ),
            name="immersed",
        )(density, base_velocity, cells, offsets, target, stiffness[None], counts)

    return jax.shard_map(
        body,
        mesh=mesh,
        in_specs=(
            P(*AXES), P(None, *AXES), P(None, ALL), P(None, ALL), P(None, ALL), P(ALL), P(ALL),
        ),
        out_specs=P(None, ALL),
        check_vma=False,
    )
```

```python
import functools

import jax
import jax.numpy as jnp
from jax import lax
from jax.experimental import pallas as pl
from jax.experimental.pallas import tpu as pltpu
from jax.sharding import PartitionSpec as P

ITERS = 3
CX, CY, CZ = 8, 8, 128
CAP = 256
WX, WY, WZ = 13, 16, 256
TZ = 144
AXES = ("gx", "gy", "gz")
ALL = ("gx", "gy", "gz")
MESH = pl.DeviceIdType.MESH
SHIFT = 0.1
F32, BF16 = jnp.float32, jnp.bfloat16

GROUPS = [(dx, dy) for dx in (-1, 0, 1) for dy in (-1, 0, 1)]
DZS = (-1, 1, 0)
ORDER = sorted(range(9), key=lambda g: abs(GROUPS[g][0]) + abs(GROUPS[g][1]))
PLANES = {-1: (0, 4), 0: (1, 12), 1: (9, 4)}
ROWS = {-1: (0, 8), 0: (0, 16), 1: (8, 8)}
TAKE = {-1: (6, 8), 0: (0, 8), 1: (0, 3)}
TAKE_BASE = {-1: (7, 8), 0: (0, 8), 1: (0, 2)}
MIDDLE = (5, 6, 7)
OUTER = (1, 2, 3, 4, 8, 9, 10, 11)
PLACE = {x: k for k, x in enumerate(OUTER + MIDDLE)}


def group_of(dx, dy):
    return (dx + 1) * 3 + dy + 1


def slot_of(dx, dy, dz):
    return group_of(dx, dy) * 3 + DZS.index(dz)


NEIGHBOURS = [
    (GROUPS[g][0], GROUPS[g][1], dz)
    for g in ORDER
    for dz in DZS
    if (GROUPS[g][0], GROUPS[g][1], dz) != (0, 0, 0)
]
NEIGHBOURS.sort(key=lambda offset: sum(map(abs, offset)))
CENTRE = group_of(0, 0)
SPANS = [PLANES[dx][1] * ROWS[dy][1] for dx, dy in GROUPS]
STARTS = [sum(SPANS[:g]) for g in range(9)]


def split(value):
    high = value.astype(BF16)
    return high, (value - high.astype(F32)).astype(BF16)


def dot3(lh, ll, rh, rl, dims):
    dot = functools.partial(
        lax.dot_general, dimension_numbers=(dims, ((), ())), preferred_element_type=F32
    )
    count = lh.shape[0]
    both = dot(jnp.concatenate([lh, ll], axis=0), rh)
    return both[:count] + (both[count:] + dot(lh, rl))


def kernel(
    sizes,
    density_in, base_in, cells_in, offsets_in, target_in, stiff_in, counts_in,
    out_ref,
    counts_ref,
    density_ref, cells_ref, offsets_ref, target_ref, stiff_ref,
    field, ftrans, pack_lo, pack_hi, spack_lo, spack_hi, pack_z_lo, pack_z_hi, mark_own,
    recv_x, recv_lo, recv_hi, srecv_x, srecv_lo, srecv_hi,
    recv_z_lo, recv_z_hi, columns, marks, main, halo, ztile, wide,
    table_h, table_l, own_h, own_l, wxy, wxy_h, wxy_l, edge_w, left_h, left_l, grid, edges, moved, plane_a, plane_b, plane_c,
    vel_h, vel_l, vecs, images, recv_v, part, recv_a, part_b, recv_b,
    loaded, send_f, got_f, send_s, got_s, send_z, got_z, send_m, got_m, send_v, got_v, send_r, got_r,
):
    size_x, size_y, size_z = sizes
    ix, iy, iz = (lax.axis_index(a) for a in AXES)

    def at(dx, dy, dz):
        return (
            lax.rem(ix + dx + size_x, size_x),
            lax.rem(iy + dy + size_y, size_y),
            lax.rem(iz + dz + size_z, size_z),
        )

    def mate(y, z):
        return (ix, lax.rem(iy + y, size_y), lax.rem(iz + z, size_z))

    def along(k):
        return (lax.rem(ix + k, size_x), iy, iz)

    loads = [
        pltpu.make_async_copy(base_in.at[c], field.at[:, c], loaded.at[c]) for c in range(3)
    ]
    loads += [
        pltpu.make_async_copy(source, target, loaded.at[3 + k])
        for k, (source, target) in enumerate(
            [
                (density_in, density_ref), (cells_in, cells_ref), (offsets_in, offsets_ref),
                (target_in, target_ref), (stiff_in, stiff_ref), (counts_in, counts_ref),
            ]
        )
    ]
    for load in loads:
        load.start()

    barrier = pltpu.get_barrier_semaphore()
    for offset in reversed(NEIGHBOURS):
        pl.semaphore_signal(barrier, inc=1, device_id=at(*offset), device_id_type=MESH)

    for load in loads:
        load.wait()
    field[:, 3] = lax.rsqrt(density_ref[...])
    ftrans[...] = field[...].reshape(4 * CX * CY, CZ).T
    pack_z_lo[...] = ftrans[CZ - 2 : CZ]
    pack_z_hi[...] = ftrans[0:4]
    for c in range(3):
        pack_lo[:, c : c + 1] = field[:, c, CY - 1 : CY]
        pack_hi[:, 2 * c : 2 * c + 2] = field[:, c, 0:2]
    spack_lo[...] = field[:, 3, CY - 2 : CY]
    spack_hi[...] = field[:, 3, 0:4]
    anchors = (ix * CX, iy * CY, iz * CZ)
    for k in range(3):
        mark_own[k : k + 1] = (cells_ref[k : k + 1] - anchors[k]).astype(F32)
    mark_own[3:6] = offsets_ref[...]
    mark_own[6:8] = jnp.zeros((2, CAP), F32)
    marks[slot_of(0, 0, 0)] = mark_own[...]

    pl.semaphore_wait(barrier, len(NEIGHBOURS))

    def remote(src, dst, send, recv, device):
        return pltpu.make_async_remote_copy(
            src_ref=src, dst_ref=dst, send_sem=send, recv_sem=recv, device_id=device,
            device_id_type=MESH,
        )

    def drain(ref, sem):
        pltpu.make_async_copy(ref, ref, sem).wait()

    def halo_copy(dx, dy):
        a, b = TAKE_BASE[-dx]
        g = group_of(-dx, -dy)
        if dy == 0:
            pair = field.at[a:b, 0:3], recv_x.at[(1 - dx) // 2, a:b]
        elif dy == 1:
            pair = pack_lo.at[a:b], recv_lo.at[1 - dx, a:b]
        else:
            pair = pack_hi.at[a:b], recv_hi.at[1 - dx, a:b]
        return remote(*pair, send_f.at[g], got_f.at[g], at(dx, dy, 0))

    def scale_copy(dx, dy):
        a, b = TAKE[-dx]
        g = group_of(-dx, -dy)
        if dy == 0:
            pair = field.at[a:b, 3], srecv_x.at[(1 - dx) // 2, a:b]
        elif dy == 1:
            pair = spack_lo.at[a:b], srecv_lo.at[1 - dx, a:b]
        else:
            pair = spack_hi.at[a:b], srecv_hi.at[1 - dx, a:b]
        return remote(*pair, send_s.at[g], got_s.at[g], at(dx, dy, 0))

    def edge_copy(dx, dy, dz):
        a, b = {-1: (0, 128), 0: (0, 256), 1: (128, 256)}[dx]
        g = group_of(-dx, -dy)
        if dz == 1:
            pair = pack_z_lo.at[:, a:b], recv_z_lo.at[g, :, a:b]
        else:
            pair = pack_z_hi.at[:, a:b], recv_z_hi.at[g, :, a:b]
        side = (1 - dz) // 2
        return remote(*pair, send_z.at[side], got_z.at[side], at(dx, dy, dz))

    around = [GROUPS[g] for g in ORDER if g != CENTRE]
    for dx, dy, dz in NEIGHBOURS:
        if dz:
            edge_copy(dx, dy, dz).start()
    for dx, dy in around:
        halo_copy(dx, dy).start()
    for dx, dy in around:
        scale_copy(dx, dy).start()
    for dx, dy, dz in NEIGHBOURS:
        back = slot_of(-dx, -dy, -dz)
        remote(mark_own, marks.at[back], send_m, got_m, at(dx, dy, dz)).start()

    own_h[...] = jnp.zeros(own_h.shape, BF16)
    own_l[...] = jnp.zeros(own_l.shape, BF16)
    ztile[...] = jnp.zeros(ztile.shape, F32)
    columns[...] = jnp.zeros(columns.shape, F32)
    main[...] = jnp.zeros(main.shape, F32)
    halo[:, :, 8:16] = jnp.zeros((WX, 4, 8, CZ), F32)
    grid[...] = jnp.zeros(grid.shape, F32)
    edges[...] = jnp.zeros(edges.shape, F32)
    vecs[...] = jnp.zeros(vecs.shape, F32)

    live = (lax.broadcasted_iota(jnp.int32, (1, CAP), 1) < counts_ref[0]).astype(F32)
    stiff = stiff_ref[...]

    def axis_table(first, rows, start, weights):
        away = (
            lax.broadcasted_iota(jnp.int32, (rows, CAP), 0).astype(F32) + float(first) - start
        )
        value = jnp.zeros((rows, CAP), F32)
        for step in range(4):
            value = jnp.where(away == float(step), weights[step], value)
        return value

    def build(g, j):
        (dx, dy), dz = GROUPS[g], DZS[j]
        mark = marks[g * 3 + j]
        fraction = mark[3:6]
        root = jnp.sqrt(1.0 + 4.0 * fraction - 4.0 * fraction * fraction)
        weights = [
            (3.0 - 2.0 * fraction - root) * 0.125,
            (3.0 - 2.0 * fraction + root) * 0.125,
            (1.0 + 2.0 * fraction + root) * 0.125,
            (1.0 + 2.0 * fraction - root) * 0.125,
        ]
        of = lambda k: [w[k : k + 1] for w in weights]
        x0, nx = PLANES[dx]
        y0, ny = ROWS[dy]
        table_x = axis_table(x0, 16, mark[0:1] + float(1 + CX * dx), of(0))
        table_y = axis_table(y0, ny, mark[1:2] + float(1 + CY * dy), of(1))
        for x in range(nx):
            rows = slice(STARTS[g] + x * ny, STARTS[g] + (x + 1) * ny)
            weight = table_x[x : x + 1] * table_y
            if dz == 0:
                wxy[rows] = weight
            else:
                high, low = split(weight)
                wxy_h[j, rows] = high
                wxy_l[j, rows] = low
        start = mark[2:3] + float(1 + CZ * dz)
        if dz == 0:
            high, low = split(axis_table(0, TZ, start, of(2)))
            table_h[g] = high
            table_l[g] = low
            if g == CENTRE:
                own_h[0:TZ] = high
                own_l[0:TZ] = low
        else:
            touched = axis_table({-1: 0, 1: CZ + 1}[dz], 8, start, of(2))[0:4]
            edge_w[2 * g + j, 0:12] = jnp.concatenate([touched] * 3, axis=0)
            edge_w[2 * g + j, 12:16] = jnp.zeros((4, CAP), F32)

    build(CENTRE, 2)

    lane = lax.broadcasted_iota(jnp.int32, (WY, CZ), 1)

    def place(takes, comps, centre, sides, low, high, low_step, high_step):
        for g, (dx, dy) in enumerate(GROUPS):
            (xa, xb), (ya, yb) = takes[dx], takes[dy]
            x0, y0 = xa + CX * dx + 2, ya + CY * dy + 2
            planes, rows = slice(x0, x0 + xb - xa), slice(y0, y0 + yb - ya)
            for k, c in enumerate(comps):
                if g == CENTRE:
                    main[planes, c, rows] = centre[:, c]
                elif dy == 0:
                    main[planes, c, rows] = sides(dx, slice(xa, xb), k)
                elif dy == -1:
                    first = k * low_step
                    main[planes, c, rows] = low[dx + 1, xa:xb, first : first + yb - ya]
                else:
                    first = k * high_step
                    main[planes, c, rows] = high[dx + 1, xa:xb, first : first + yb - ya]

    def widened(x, c):
        turned = pltpu.roll(main[x, c], 2, 1)
        edge = halo[x, c]
        head = jnp.where(lane < 2, edge, turned)
        tail = jnp.where(lane < 2, turned, jnp.where(lane < 5, edge, 0.0))
        return jnp.concatenate([head, tail], axis=1)

    for dx, dy in around:
        halo_copy(dx, dy).wait_recv()
    place(
        TAKE_BASE, (0, 1, 2), field, lambda dx, planes, k: recv_x[(dx + 1) // 2, planes, k],
        recv_lo, recv_hi, 1, 2,
    )
    drain(recv_z_lo.at[0:6], got_z.at[0])
    drain(recv_z_hi.at[0:6], got_z.at[1])
    for g, (dx, dy) in enumerate(GROUPS):
        (xa, xb), (ya, yb) = TAKE[dx], TAKE[dy]
        x0, y0 = xa + CX * dx + 2, ya + CY * dy + 2
        columns[0:2] = recv_z_lo[g]
        columns[2:6] = recv_z_hi[g]
        ztile[:, :, :, 0:8] = columns[...].T.reshape(CX, 4, CY, 8)
        halo[x0 : x0 + xb - xa, :, y0 : y0 + yb - ya] = ztile[xa:xb, :, ya:yb]

    def interpolate(planes):
        first, count = PLACE[planes[0]], len(planes)
        span = count * WY
        rows = dot3(
            vel_h[:, first : first + count].reshape(3 * span, WZ),
            vel_l[:, first : first + count].reshape(3 * span, WZ),
            own_h[...], own_l[...], ((1,), (0,)),
        )
        starts = [STARTS[CENTRE] + (x - 1) * WY for x in planes]
        weight = jnp.concatenate([wxy[start : start + WY] for start in starts], axis=0)
        return [
            jnp.sum(rows[c * span : (c + 1) * span] * weight, axis=0, keepdims=True)
            for c in range(3)
        ]

    for x in range(1, 12):
        for c in range(3):
            high, low = split(widened(x, c))
            vel_h[c, PLACE[x]] = high
            vel_l[c, PLACE[x]] = low
    for c, value in enumerate(interpolate(OUTER + MIDDLE)):
        vecs[0, c : c + 1] = live * (target_ref[c : c + 1] - value)

    def send_vector(a):
        for dx, dy, dz in NEIGHBOURS:
            back = slot_of(-dx, -dy, -dz)
            remote(
                vecs.at[a], recv_v.at[a, back], send_v.at[a], got_v.at[a, abs(dx) + abs(dy) + abs(dz) - 1],
                at(dx, dy, dz),
            ).start()
        recv_v[a, slot_of(0, 0, 0)] = vecs[a]

    part_row = lax.broadcasted_iota(jnp.int32, (16, CAP), 0)

    def spread_inner(a, g):
        span = SPANS[g]
        vector = recv_v[a, 3 * g + 2]
        weight = wxy[STARTS[g] : STARTS[g] + span]
        for c in range(3):
            high, low = split(weight * vector[c : c + 1])
            left_h[c * span : (c + 1) * span] = high
            left_l[c * span : (c + 1) * span] = low
        return dot3(left_h[0 : 3 * span], left_l[0 : 3 * span], table_h[g], table_l[g], ((1,), (1,)))

    def spread_edges(a, g):
        rows = slice(STARTS[g], STARTS[g] + SPANS[g])
        sides = []
        for j in range(2):
            vector = recv_v[a, 3 * g + j]
            value = jnp.where(
                part_row < 4, vector[0:1], jnp.where(part_row < 8, vector[1:2], vector[2:3])
            )
            high, low = split(edge_w[2 * g + j] * value)
            sides.append(dot3(high, low, wxy_h[j, rows], wxy_l[j, rows], ((1,), (1,))))
        return jnp.concatenate(sides, axis=0).T

    def add_inner(a, g):
        (dx, dy), span = GROUPS[g], SPANS[g]
        x0, nx = PLANES[dx]
        y0, ny = ROWS[dy]
        total = spread_inner(a, g)
        for c in range(3):
            at_place = (c, slice(x0, x0 + nx), slice(y0, y0 + ny), slice(0, TZ))
            grid[at_place] += total[c * span : (c + 1) * span].reshape(nx, ny, TZ)

    def add_edges(a, g):
        dx, dy = GROUPS[g]
        x0, nx = PLANES[dx]
        y0, ny = ROWS[dy]
        edges[x0 : x0 + nx, y0 : y0 + ny, 0:32] += spread_edges(a, g).reshape(nx, ny, 32)

    def spread(a, middle):
        far = [abs(dx) + abs(dy) for dx, dy in GROUPS]
        grid[:, :, :, 0:TZ] = jnp.zeros((3, WX, WY, TZ), F32)
        edges[:, :, 0:32] = jnp.zeros((WX, WY, 32), F32)
        kept = None
        for hops, messages in enumerate((0, 6, 12, 8)):
            if hops:
                drain(recv_v.at[a, 0:messages], got_v.at[a, hops - 1])
            if hops == 3:
                kept = middle()
            for g in range(9):
                if far[g] == hops:
                    add_inner(a, g)
            for g in range(9):
                if far[g] == hops - 1:
                    add_edges(a, g)
        return kept

    def shifts(value, axis):
        length = value.shape[axis]
        return pltpu.roll(value, 1, axis), pltpu.roll(value, length - 1, axis)

    def both(value, axis):
        before, after = shifts(value, axis)
        return before + after

    def stream(last, planes, outputs, energy):
        inner = range(2, 10) if last else range(1, 12)
        for x in planes:
            scale = wide[x]
            edge = edges[x]
            values = []
            for c in range(3):
                head = grid[c, x, :, 0:CZ] + jnp.where(
                    lane < 4, pltpu.roll(edge, CZ - 4 * c, 1) if c else edge, 0.0
                )
                tail = grid[c, x, :, CZ:] + jnp.where(
                    (lane > 0) & (lane < 5), pltpu.roll(edge, CZ - 15 - 4 * c, 1), 0.0
                )
                values.append(scale * jnp.concatenate([head, tail], axis=1))
            m0, m1, m2 = values
            moved[0, x], moved[1, x], moved[2, x] = m0, m1, m2
            before, after = shifts(m0, 0)
            sy0, dy0 = before + after, before - after
            before, after = shifts(m1, 0)
            sy1, dy1 = before + after, before - after
            before, after = shifts(m0, 1)
            sz0, dz0 = before + after, before - after
            before, after = shifts(m2, 1)
            sz2, dz2 = before + after, before - after
            plane_a[0, x] = 2.0 * m0 + sy0 + sz0
            plane_b[0, x] = dy1 + dz2
            plane_a[1, x] = sy1
            plane_b[1, x] = dy0
            plane_a[2, x] = sz2
            plane_b[2, x] = dz0
            if x in inner:
                before, after = shifts(dz2, 0)
                plane_c[0, x] = 2.0 * sy1 + both(sy1, 1) + (before - after)
                before, after = shifts(dy1, 1)
                plane_c[1, x] = 2.0 * sz2 + both(sz2, 0) + (before - after)

        for x in outputs:
            half = wide[x] * 0.5
            for c in range(3):
                post = plane_a[c, x - 1] + plane_a[c, x + 1] + plane_b[c, x - 1] - plane_b[c, x + 1]
                if c:
                    post = post + plane_c[c - 1, x]
                response = moved[c, x] + post * (1.0 / 12.0)
                if last:
                    energy = energy + moved[c, x] * response
                else:
                    high, low = split(half * response)
                    vel_h[c, PLACE[x]] = high
                    vel_l[c, PLACE[x]] = low
        return energy

    lane_row = lax.broadcasted_iota(jnp.int32, (1, 128), 1)
    me = iy * size_z + iz
    mates = size_y * size_z - 1
    far_mates = [(y, z) for y in range(size_y) for z in range(size_z) if (y, z) != (0, 0)]
    far_mates.sort(key=lambda k: -(min(k[0], size_y - k[0]) / 2 + min(k[1], size_z - k[1])))

    def sum_plane(k, row):
        part[k] = row
        recv_a[k, me] = row
        for other in far_mates:
            remote(part.at[k], recv_a.at[k, me], send_r.at[k], got_r.at[k], mate(*other)).start()

    def sum_along(k):
        drain(recv_a.at[k, 0:mates], got_r.at[k])
        row = jnp.sum(recv_a[k], axis=0)
        part_b[k] = row
        recv_b[k, ix] = row
        for other in sorted(range(1, size_x), key=lambda k: -min(k, size_x - k)):
            remote(
                part_b.at[k], recv_b.at[k, ix], send_r.at[2 + k], got_r.at[2 + k], along(other)
            ).start()

    def summed(k):
        drain(recv_b.at[k, 0 : size_x - 1], got_r.at[2 + k])
        return jnp.sum(recv_b[k], axis=0)

    for a in range(ITERS):
        send_vector(a)
        if a == 0:
            for dx, dy in around:
                scale_copy(dx, dy).wait_recv()
            place(
                TAKE, (3,), field, lambda dx, planes, k: srecv_x[(dx + 1) // 2, planes],
                srecv_lo, srecv_hi, 0, 0,
            )
            for x in range(WX):
                wide[x] = widened(x, 3)
            drain(marks.at[0:26], got_m)
            for g in ORDER:
                for j in range(3):
                    if (g, j) != (CENTRE, 2):
                        build(g, j)
        last = a == ITERS - 1
        if last:
            v = [vecs[k, 0:3] for k in range(3)]
            w = [images[k, 0:3] for k in range(2)]
            pairs = [(v[0], w[0]), (v[0], w[1]), (v[2], w[0]), (v[1], w[1]), (v[2], w[1])]
            pairs = pairs + [(v[0], v[j]) for j in range(3)]
            row = jnp.zeros((1, 128), F32)
            for k, (left, right) in enumerate(pairs):
                row = jnp.where(lane_row == k, jnp.sum(left * right), row)
            sum_plane(0, row)

        def middle():
            return None

        kept = spread(a, middle)
        if last:
            sum_along(0)
            energy = stream(last, range(1, 11), range(2, 10), jnp.zeros((WY, WZ), F32))
        else:
            stream(last, range(WX), range(1, 12), None)
            for c, value in enumerate(interpolate(OUTER + MIDDLE)):
                vector = vecs[a, c : c + 1]
                image = live * (value + stiff * vector)
                images[a, c : c + 1] = image
                vecs[a + 1, c : c + 1] = image - SHIFT * vector

    inside = lambda axis, size: (
        lax.broadcasted_iota(jnp.int32, (WY, WZ), axis) - 2
    ).astype(jnp.uint32) < size
    energy = jnp.where(inside(0, CY) & inside(1, CZ), energy, 0.0)
    own = jnp.sum(0.5 * energy, axis=0, keepdims=True)
    own = own + jnp.sum(stiff * v[2] * v[2], axis=0, keepdims=True)
    sum_plane(1, own[:, 0:128] + own[:, 128:256])
    total = summed(0)
    h00, h01, h02, h11, h12, b0, b1, b2 = (
        jnp.sum(jnp.where(lane_row == k, total, 0.0), axis=1, keepdims=True) for k in range(8)
    )

    def over(top, pivot, size):
        fine = pivot > 1e-7 * size
        return jnp.where(fine, top / jnp.where(fine, pivot, 1.0), 0.0)

    l10 = over(h01, h00, h00)
    l20 = over(h02, h00, h00)
    d1 = h11 - l10 * h01
    e12 = h12 - l10 * h02
    l21 = over(e12, d1, h11)
    less = h02 * l20 + l21 * e12
    z1 = b1 - l10 * b0
    z2 = b2 - l20 * b0 - l21 * z1
    y1 = over(z1, d1, h11)
    y0 = over(b0, h00, h00) - l10 * y1
    first = y0 * v[0] + y1 * v[1]
    second = v[2] - l21 * v[1] + (l10 * l21 - l20) * v[0]
    sum_along(1)
    h22 = jnp.sum(summed(1), axis=1, keepdims=True)
    out_ref[...] = first + over(z2, h22 - less, h22) * second

    for dx, dy in GROUPS:
        if (dx, dy) != (0, 0):
            halo_copy(dx, dy).wait_send()
            scale_copy(dx, dy).wait_send()
    drain(recv_z_lo.at[0:6], send_z.at[0])
    drain(recv_z_hi.at[0:6], send_z.at[1])
    drain(marks.at[0:26], send_m)
    for a in range(ITERS):
        drain(recv_v.at[a, 0:26], send_v.at[a])
    for k in range(2):
        drain(recv_a.at[k, 0:mates], send_r.at[k])
        drain(recv_b.at[k, 0 : size_x - 1], send_r.at[2 + k])


def solution(mesh):
    sizes = tuple(mesh.shape[a] for a in AXES)
    plane = sizes[1] * sizes[2]

    def body(density, base_velocity, cells, offsets, target, stiffness, counts):
        vmem = pl.BlockSpec(memory_space=pltpu.VMEM)
        return pl.pallas_call(
            functools.partial(kernel, sizes),
            out_shape=jax.ShapeDtypeStruct((3, CAP), F32),
            in_specs=[pl.BlockSpec(memory_space=pl.ANY)] * 7,
            out_specs=vmem,
            scratch_shapes=[
                pltpu.SMEM((1,), jnp.int32),
                pltpu.VMEM((CX, CY, CZ), F32),
                pltpu.VMEM((3, CAP), jnp.int32),
                pltpu.VMEM((3, CAP), F32),
                pltpu.VMEM((3, CAP), F32),
                pltpu.VMEM((1, CAP), F32),
                pltpu.VMEM((CX, 4, CY, CZ), F32),
                pltpu.VMEM((CZ, 4 * CX * CY), F32),
                pltpu.VMEM((CX, 4, CZ), F32),
                pltpu.VMEM((CX, 8, CZ), F32),
                pltpu.VMEM((CX, 2, CZ), F32),
                pltpu.VMEM((CX, 4, CZ), F32),
                pltpu.VMEM((2, 4 * CX * CY), F32),
                pltpu.VMEM((4, 4 * CX * CY), F32),
                pltpu.VMEM((8, CAP), F32),
                pltpu.VMEM((2, CX, 3, CY, CZ), F32),
                pltpu.VMEM((3, CX, 4, CZ), F32),
                pltpu.VMEM((3, CX, 8, CZ), F32),
                pltpu.VMEM((2, CX, CY, CZ), F32),
                pltpu.VMEM((3, CX, 2, CZ), F32),
                pltpu.VMEM((3, CX, 4, CZ), F32),
                pltpu.VMEM((9, 2, 4 * CX * CY), F32),
                pltpu.VMEM((9, 4, 4 * CX * CY), F32),
                pltpu.VMEM((8, 4 * CX * CY), F32),
                pltpu.VMEM((27, 8, CAP), F32),
                pltpu.VMEM((WX, 4, WY, CZ), F32),
                pltpu.VMEM((WX, 4, WY, CZ), F32),
                pltpu.VMEM((CX, 4, CY, CZ), F32),
                pltpu.VMEM((WX, WY, WZ), F32),
                pltpu.VMEM((9, TZ, CAP), BF16),
                pltpu.VMEM((9, TZ, CAP), BF16),
                pltpu.VMEM((WZ, CAP), BF16),
                pltpu.VMEM((WZ, CAP), BF16),
                pltpu.VMEM((sum(SPANS), CAP), F32),
                pltpu.VMEM((2, sum(SPANS), CAP), BF16),
                pltpu.VMEM((2, sum(SPANS), CAP), BF16),
                pltpu.VMEM((18, 16, CAP), F32),
                pltpu.VMEM((3 * max(SPANS), CAP), BF16),
                pltpu.VMEM((3 * max(SPANS), CAP), BF16),
                pltpu.VMEM((3, WX, WY, WZ), F32),
                pltpu.VMEM((WX, WY, CZ), F32),
                pltpu.VMEM((3, WX, WY, WZ), F32),
                pltpu.VMEM((3, WX, WY, WZ), F32),
                pltpu.VMEM((3, WX, WY, WZ), F32),
                pltpu.VMEM((2, WX, WY, WZ), F32),
                pltpu.VMEM((3, 11, WY, WZ), BF16),
                pltpu.VMEM((3, 11, WY, WZ), BF16),
                pltpu.VMEM((ITERS + 1, 4, CAP), F32),
                pltpu.VMEM((ITERS, 4, CAP), F32),
                pltpu.VMEM((ITERS, 27, 4, CAP), F32),
                pltpu.VMEM((2, 1, 128), F32),
                pltpu.VMEM((2, plane, 1, 128), F32),
                pltpu.VMEM((2, 1, 128), F32),
                pltpu.VMEM((2, sizes[0], 1, 128), F32),
                pltpu.SemaphoreType.DMA((9,)),
                pltpu.SemaphoreType.DMA((9,)),
                pltpu.SemaphoreType.DMA((9,)),
                pltpu.SemaphoreType.DMA((9,)),
                pltpu.SemaphoreType.DMA((9,)),
                pltpu.SemaphoreType.DMA((2,)),
                pltpu.SemaphoreType.DMA((2,)),
                pltpu.SemaphoreType.DMA,
                pltpu.SemaphoreType.DMA,
                pltpu.SemaphoreType.DMA((ITERS,)),
                pltpu.SemaphoreType.DMA((ITERS, 3)),
                pltpu.SemaphoreType.DMA((4,)),
                pltpu.SemaphoreType.DMA((4,)),
            ],
            compiler_params=pltpu.CompilerParams(
                collective_id=0, has_side_effects=True, vmem_limit_bytes=60 * 1024 * 1024
            ),
            name="immersed",
        )(density, base_velocity, cells, offsets, target, stiffness[None], counts)

    return jax.shard_map(
        body,
        mesh=mesh,
        in_specs=(
            P(*AXES), P(None, *AXES), P(None, ALL), P(None, ALL), P(None, ALL), P(ALL), P(ALL),
        ),
        out_specs=P(None, ALL),
        check_vma=False,
    )
```
